32 devices in a mesh: ha: 4 (over y, x), wa: 8 (over z, core).
Axes of the slice: x: 2, y: 2, z: 4, core: 2. Of those that a mesh axis runs over, the one named last changes fastest.
Arguments:
- tokens: bfloat16 [112, 224, 384], P('ha', 'wa'), may hold values from -8 to 8
- cotangent: bfloat16 [112, 224, 384], P('ha', 'wa'), may hold values from -8 to 8
- w_qkv: bfloat16 [384, 1152], replicated, may hold values from -0.3125 to 0.3125
- w_proj: bfloat16 [384, 384], replicated, may hold values from -0.3125 to 0.3125
- w_fc1: bfloat16 [384, 1536], replicated, may hold values from -0.3125 to 0.3125
- w_fc2: bfloat16 [1536, 384], replicated, may hold values from -0.15625 to 0.15625
- bias_table: float32 [169, 12], replicated, may hold values from -4 to 280
- rel_index: int32 [49, 49], replicated, may hold values from 0 to 168, as said below
- region: int32 [112, 224], P('ha', 'wa'), may hold values from 0 to 15, as said below
Outputs:
- block_out: bfloat16 [112, 224, 384], P('ha', 'wa')
- token_grad: bfloat16 [112, 224, 384], P('ha', 'wa')
- grad_qkv: float32 [384, 1152], replicated
- grad_proj: float32 [384, 384], replicated
- grad_fc1: float32 [384, 1536], replicated
- grad_fc2: float32 [1536, 384], replicated
- grad_table: float32 [169, 12], replicated
The draws below stay inside these ranges and needn't reach their ends.
Inputs may be any that keep to these rules, and one draw needn't show every extreme that they name: `rel_index`: pairs of window positions with the same offset share an entry, pairs with different offsets have different entries. `region`: the crop id of the token at each position of the shifted grid.
All inputs are finite; a program needn't handle non-finite values.
Results may differ from the reference program's by a relative error of at most 0.016.
Values may be sent and summed in bfloat16 or wider, within the bound.
A program may use at most 128 MiB of HBM per device.

```python
import math
import jax
import jax.numpy as jnp
from jax import lax

C = 384
HEADS = 12
FFN = 1536
SIDE = 7
SHIFT = 3
CROPS = 4
HEAD_DIM = 32
WINDOW = 49
TABLE = 169
NH = 112
NW = 224
PARAMS = 1771500


def field_drawn(key, salt):
    values = jax.random.normal(jax.random.fold_in(key, salt), (NH, NW, C), jnp.float32)
    return jnp.clip(values, -8.0, 8.0).astype(jnp.bfloat16)


def draw_tokens(key, part):
    return field_drawn(key, 31)


def draw_cotangent(key, part):
    return field_drawn(key, 41)


def label_order(key):
    return jax.random.permutation(jax.random.fold_in(key, 7), TABLE).astype(jnp.int32)


def draw_rel_index(key, part):
    order = label_order(key)
    places = jnp.arange(WINDOW, dtype=jnp.int32)
    offset_rows = places[:, None] // SIDE - places[None, :] // SIDE + SIDE - 1
    offset_cols = places[:, None] % SIDE - places[None, :] % SIDE + SIDE - 1
    return order[offset_rows * (2 * SIDE - 1) + offset_cols]


def draw_bias_table(key, part):
    values = jax.random.normal(jax.random.fold_in(key, 21), (TABLE, HEADS), jnp.float32)
    return jnp.clip(values, -4.0, 4.0)


def crop_of(places, cuts):
    return jnp.sum((places[:, None] >= cuts[None, :]).astype(jnp.int32), 1)


def draw_region(key, part):
    row_cuts = jax.random.randint(jax.random.fold_in(key, 3), (CROPS - 1,), 1, NH, dtype=jnp.int32)
    col_cuts = jax.random.randint(jax.random.fold_in(key, 4), (CROPS - 1,), 1, NW, dtype=jnp.int32)
    row_places = (jnp.arange(NH, dtype=jnp.int32) + SHIFT) % NH
    col_places = (jnp.arange(NW, dtype=jnp.int32) + SHIFT) % NW
    return crop_of(row_places, row_cuts)[:, None] * CROPS + crop_of(col_places, col_cuts)[None, :]


def scatter_about(own_key, shape, deviation, bound, held_as=jnp.bfloat16):
    return jnp.clip(deviation * jax.random.normal(own_key, shape, jnp.float32), -bound, bound).astype(held_as)


def setup_inputs(seed: int = 0) -> dict:
    splits = jax.random.split(jax.random.key(seed), 10)
    return {
        "tokens": draw_tokens(jax.random.fold_in(splits[9], 71), 0),
        "cotangent": draw_cotangent(jax.random.fold_in(splits[9], 71), 0),
        "w_qkv": scatter_about(splits[2], (C, 3 * C), C ** -0.5, 0.3125),
        "w_proj": scatter_about(splits[3], (C, C), C ** -0.5, 0.3125),
        "w_fc1": scatter_about(splits[4], (C, FFN), C ** -0.5, 0.3125),
        "w_fc2": scatter_about(splits[5], (FFN, C), FFN ** -0.5, 0.15625),
        "bias_table": draw_bias_table(jax.random.fold_in(splits[9], 71), 0),
        "rel_index": draw_rel_index(jax.random.fold_in(splits[9], 71), 0),
        "region": draw_region(jax.random.fold_in(splits[9], 71), 0),
    }


epsilon = 1e-05
highest = lax.Precision.HIGHEST

def rounded(values):
    return lax.optimization_barrier(values.astype(jnp.bfloat16)).astype(jnp.float32)

def normalize(values):
    average = lax.optimization_barrier(jnp.mean(values, -1, keepdims=True))
    centred = values - average
    inverse = lax.rsqrt(lax.optimization_barrier(jnp.mean(centred * centred, -1, keepdims=True)) + epsilon)
    return (centred * inverse, inverse)

def normalize_back(normal_rows, inverse, upstream):
    up_mean = lax.optimization_barrier(jnp.mean(upstream, -1, keepdims=True))
    cross_mean = lax.optimization_barrier(jnp.mean(upstream * normal_rows, -1, keepdims=True))
    return inverse * (upstream - up_mean - normal_rows * cross_mean)

def gelu_slope(pre_act):
    normal_cdf = 0.5 * (1.0 + lax.erf(pre_act * 2.0 ** (-0.5)))
    return normal_cdf + pre_act * jnp.exp(-0.5 * pre_act * pre_act) * (2.0 * math.pi) ** (-0.5)

def to_windows(grid_in):
    row_count, col_count = (grid_in.shape[0], grid_in.shape[1])
    shaped = grid_in.reshape(row_count // SIDE, SIDE, col_count // SIDE, SIDE, -1)
    return shaped.transpose(0, 2, 1, 3, 4).reshape(row_count // SIDE, col_count // SIDE, WINDOW, -1)

def from_windows(grid_in):
    band_count, across, channels = (grid_in.shape[0], grid_in.shape[1], grid_in.shape[3])
    shaped = grid_in.reshape(band_count, across, SIDE, SIDE, channels)
    return shaped.transpose(0, 2, 1, 3, 4).reshape(band_count * SIDE, across * SIDE, channels)

def attend(qkv_win, region_win, pos_bias):
    win_count = qkv_win.shape[0]
    parts_qkv = qkv_win.reshape(win_count, WINDOW, 3, HEADS, HEAD_DIM).astype(jnp.float32)
    queries, keys_in, values = (parts_qkv[:, :, 0], parts_qkv[:, :, 1], parts_qkv[:, :, 2])
    scores = jnp.einsum('wihd,wjhd->whij', queries, keys_in, precision=highest) * HEAD_DIM ** (-0.5) + pos_bias[None]
    same_region = region_win[:, :, None] == region_win[:, None, :]
    scores = jnp.where(same_region[:, None], scores, -1e+30)
    exponent = jnp.exp(scores - lax.optimization_barrier(jnp.max(scores, -1, keepdims=True)))
    attn_probs = exponent / lax.optimization_barrier(jnp.sum(exponent, -1, keepdims=True))
    weighted = jnp.einsum('whij,wjhd->wihd', rounded(attn_probs), values, precision=highest)
    return (weighted.reshape(win_count, WINDOW, HEADS * HEAD_DIM).astype(jnp.bfloat16), attn_probs)

def attend_back(qkv_win, attn_probs, upstream):
    win_count = qkv_win.shape[0]
    parts_qkv = qkv_win.reshape(win_count, WINDOW, 3, HEADS, HEAD_DIM).astype(jnp.float32)
    queries, keys_in, values = (parts_qkv[:, :, 0], parts_qkv[:, :, 1], parts_qkv[:, :, 2])
    grad_out = upstream.reshape(win_count, WINDOW, HEADS, HEAD_DIM).astype(jnp.float32)
    grad_probs = jnp.einsum('wihd,wjhd->whij', grad_out, values, precision=highest)
    grad_values = jnp.einsum('whij,wihd->wjhd', rounded(attn_probs), grad_out, precision=highest)
    grad_scores = attn_probs * (grad_probs - lax.optimization_barrier(jnp.sum(attn_probs * grad_probs, -1, keepdims=True)))
    bias_grad = lax.optimization_barrier(jnp.sum(grad_scores, 0))
    scaled = rounded(grad_scores * HEAD_DIM ** (-0.5))
    grad_queries = jnp.einsum('whij,wjhd->wihd', scaled, keys_in, precision=highest)
    grad_keys = jnp.einsum('whij,wihd->wjhd', scaled, queries, precision=highest)
    stacked = jnp.stack([grad_queries, grad_keys, grad_values], 2)
    return (stacked.reshape(win_count, WINDOW, 3 * HEADS * HEAD_DIM).astype(jnp.bfloat16), bias_grad)

def reference(tokens, cotangent, w_qkv, w_proj, w_fc1, w_fc2, bias_table, rel_index, region):
    row_count, col_count, channels = tokens.shape
    lookup = (rel_index.reshape(-1)[:, None] == jnp.arange(TABLE, dtype=jnp.int32)[None, :]).astype(jnp.float32)
    pos_bias = jnp.dot(lookup, bias_table, precision=highest).T.reshape(HEADS, WINDOW, WINDOW)
    token_f32 = tokens.astype(jnp.float32)
    first_norm, first_scale = normalize(token_f32)
    shifted = jnp.roll(first_norm.astype(jnp.bfloat16), (-SHIFT, -SHIFT), (0, 1))
    flat_shift = shifted.reshape(-1, channels)
    qkv_tok = jnp.dot(flat_shift, w_qkv, preferred_element_type=jnp.float32).astype(jnp.bfloat16)
    qkv_win = to_windows(qkv_tok.reshape(row_count, col_count, 3 * channels))
    region_win = to_windows(region[..., None])[..., 0]

    def forward_band(operands):
        return attend(operands[0], operands[1], pos_bias)
    attn_win, attn_probs = lax.map(forward_band, (qkv_win, region_win))
    attn_tok = from_windows(attn_win).reshape(-1, channels)
    projected = jnp.dot(attn_tok, w_proj, preferred_element_type=jnp.float32).astype(jnp.bfloat16)
    middle = token_f32 + jnp.roll(projected.reshape(row_count, col_count, channels), (SHIFT, SHIFT), (0, 1)).astype(jnp.float32)
    second_norm, second_scale = normalize(middle)
    normed_low = second_norm.astype(jnp.bfloat16).reshape(-1, channels)
    pre_act = jnp.dot(normed_low, w_fc1, preferred_element_type=jnp.float32)
    activated = jax.nn.gelu(pre_act, approximate=False).astype(jnp.bfloat16)
    block_out = (middle + jnp.dot(activated, w_fc2, preferred_element_type=jnp.float32).reshape(row_count, col_count, channels)).astype(jnp.bfloat16)
    upstream = cotangent.reshape(-1, channels)
    raw_fc2 = jnp.dot(activated.T, upstream, preferred_element_type=jnp.float32)
    grad_pre = (jnp.dot(upstream, w_fc2.T, preferred_element_type=jnp.float32) * gelu_slope(pre_act)).astype(jnp.bfloat16)
    raw_fc1 = jnp.dot(normed_low.T, grad_pre, preferred_element_type=jnp.float32)
    grad_second = jnp.dot(grad_pre, w_fc1.T, preferred_element_type=jnp.float32).reshape(row_count, col_count, channels)
    grad_mid = cotangent.astype(jnp.float32) + normalize_back(second_norm, second_scale, grad_second)
    back_rolled = jnp.roll(grad_mid.astype(jnp.bfloat16), (-SHIFT, -SHIFT), (0, 1)).reshape(-1, channels)
    raw_proj = jnp.dot(attn_tok.T, back_rolled, preferred_element_type=jnp.float32)
    grad_attn = jnp.dot(back_rolled, w_proj.T, preferred_element_type=jnp.float32).astype(jnp.bfloat16)
    attn_back = to_windows(grad_attn.reshape(row_count, col_count, channels))

    def backward_band(operands):
        return attend_back(operands[0], operands[1], operands[2])
    qkv_grads, bias_parts = lax.map(backward_band, (qkv_win, attn_probs, attn_back))
    bias_grad = lax.optimization_barrier(jnp.sum(bias_parts, 0))
    raw_table = jnp.dot(lookup.T, bias_grad.reshape(HEADS, -1).T, precision=highest)
    qkv_back = from_windows(qkv_grads).reshape(-1, 3 * channels)
    raw_qkv = jnp.dot(flat_shift.T, qkv_back, preferred_element_type=jnp.float32)
    grad_shift = jnp.dot(qkv_back, w_qkv.T, preferred_element_type=jnp.float32).astype(jnp.bfloat16)
    grad_normed = jnp.roll(grad_shift.reshape(row_count, col_count, channels), (SHIFT, SHIFT), (0, 1))
    token_grad = (grad_mid + normalize_back(first_norm, first_scale, grad_normed.astype(jnp.float32))).astype(jnp.bfloat16)
    raw = (raw_qkv, raw_proj, raw_fc1, raw_fc2, raw_table)
    norm_sq = jnp.sum(jnp.stack([jnp.sum(gradient * gradient) for gradient in raw]))
    factor = jnp.minimum(1.0, math.sqrt(PARAMS) / (jnp.sqrt(norm_sq) + 1e-06))
    return (block_out, token_grad, raw_qkv * factor, raw_proj * factor, raw_fc1 * factor, raw_fc2 * factor, raw_table * factor)
```

```python
import functools
import math

import jax
import jax.numpy as jnp
from jax import lax
from jax.experimental import pallas as pl
from jax.experimental.pallas import tpu as pltpu
from jax.sharding import PartitionSpec as P

HEADS = 12
SIDE = 7
SHIFT = 3
HEAD_DIM = 32
TABLE = 169
PARAMS = 1771500
CELL = 8
SLOTS = CELL * CELL
GROUP = 4
LANES = GROUP * HEAD_DIM
GROUPS = HEADS // GROUP
FFN_CHUNKS = 3
SUB = 16
LANE = 128
TILE = SUB * LANE
STREAMS = (4, 2)
MESH = pl.DeviceIdType.MESH

epsilon = 1e-05
highest = lax.Precision.HIGHEST
f32 = jnp.float32
bf16 = jnp.bfloat16


def from_behind(x, axis, by):
    count = lax.axis_size(axis)
    return lax.ppermute(x, axis, [(i, (i + by) % count) for i in range(count)])


def to_shifted(grid_in):
    lower_rim = from_behind(grid_in[:SHIFT], "ha", -1)
    taller = jnp.concatenate([grid_in[SHIFT:], lower_rim], 0)
    right_rim = from_behind(taller[:, :SHIFT], "wa", -1)
    return jnp.concatenate([taller[:, SHIFT:], right_rim], 1)


def from_shifted(grid_in):
    upper_rim = from_behind(grid_in[-SHIFT:], "ha", 1)
    taller = jnp.concatenate([upper_rim, grid_in[:-SHIFT]], 0)
    left_rim = from_behind(taller[:, -SHIFT:], "wa", 1)
    return jnp.concatenate([left_rim, taller[:, :-SHIFT]], 1)


def to_cells(grid_in, fill):
    rows, cols, channels = grid_in.shape
    split = grid_in.reshape(rows // SIDE, SIDE, cols // SIDE, SIDE, channels)
    extra = CELL - SIDE
    padded = jnp.pad(
        split, ((0, 0), (0, extra), (0, 0), (0, extra), (0, 0)), constant_values=fill
    )
    return padded.transpose(0, 2, 1, 3, 4).reshape(-1, channels)


def from_cells(flat, rows, cols):
    split = flat.reshape(rows // SIDE, cols // SIDE, CELL, CELL, -1)[:, :, :SIDE, :SIDE]
    return split.transpose(0, 2, 1, 3, 4).reshape(rows, cols, -1)


def normalize(values):
    average = jnp.mean(values, -1, keepdims=True)
    centred = values - average
    inverse = lax.rsqrt(jnp.mean(centred * centred, -1, keepdims=True) + epsilon)
    return (centred * inverse, inverse)


def normalize_back(normal_rows, inverse, upstream):
    up_mean = jnp.mean(upstream, -1, keepdims=True)
    cross_mean = jnp.mean(upstream * normal_rows, -1, keepdims=True)
    return inverse * (upstream - up_mean - normal_rows * cross_mean)


def product(left, right, left_dim, right_dim):
    return lax.dot_general(
        left, right, (((left_dim,), (right_dim,)), ((), ())), preferred_element_type=f32
    )


def head_mask():
    shape = (GROUP * SLOTS, LANES)
    row_head = lax.broadcasted_iota(jnp.int32, shape, 0) // SLOTS
    lane_head = lax.broadcasted_iota(jnp.int32, shape, 1) // HEAD_DIM
    return (row_head == lane_head).astype(f32)


def stack_heads(rows, mask):
    return jnp.concatenate([rows] * GROUP, 0) * mask


def gather_heads(stacked, mask):
    kept = stacked * mask
    total = kept[:SLOTS]
    for head in range(1, GROUP):
        total = total + kept[head * SLOTS : (head + 1) * SLOTS]
    return total


def to_tiles(values, tiles_ref, at):
    rows, lanes = values.shape
    high = rows // SUB
    low = values.astype(bf16)
    for column in range(lanes // LANE):
        block = low[:, column * LANE : (column + 1) * LANE].reshape(high, SUB, LANE)
        tiles_ref[at + column * high : at + (column + 1) * high] = block


def from_tiles(tiles_ref, at, rows, column):
    high = rows // SUB
    block = tiles_ref[at + column * high : at + (column + 1) * high]
    return block.reshape(rows, LANE).astype(f32)


def strides_of(size):
    return [1 << i for i in range(size.bit_length() - 1)]


def link_orders(across_ha, across_wa):
    first, *far = [("wa", stride) for stride in strides_of(across_wa)]
    near = [("ha", stride) for stride in strides_of(across_ha)]
    return ([first] + near + far, [first] + near[::-1] + far)


def split_streams(group, tiles, devices, parts, orders):
    units = tiles // devices
    streams = []
    base = 0
    for part in range(parts):
        size = (units // parts + (part < units % parts)) * devices
        if size:
            streams.append((group, base, size, orders[part % len(orders)]))
        base += size
    return streams


def padded_tiles(tiles, devices):
    return -(-tiles // devices) * devices


def chunk_of(count):
    return max(size for size in range(1, 17) if count % size == 0)


class Exchange:
    def __init__(self, streams, sources, sums, landing, totals, send_sem, recv_sem):
        self.streams = streams
        self.sources, self.sums, self.landing, self.totals = sources, sums, landing, totals
        self.send_sem, self.recv_sem = send_sem, recv_sem
        self.rounds = len(streams[0][3])
        self.copies = []
        self.places = []
        for group, base, size, order in streams:
            places = []
            low = base
            for step, (axis, stride) in enumerate(order):
                half = size >> (step + 1)
                me = lax.axis_index(axis)
                bit = (me // stride) % 2
                partner = {axis: me + stride - 2 * stride * bit}
                keep = low + bit * half
                give = low + half - bit * half
                places.append((partner, keep, give, half))
                low = keep
            self.places.append(places)

    def greet(self):
        barrier = pltpu.get_barrier_semaphore()
        partners = {link: place[0] for stream, places in zip(self.streams, self.places) for link, place in zip(stream[3], places)}
        for partner in partners.values():
            pl.semaphore_signal(barrier, inc=1, device_id=partner, device_id_type=MESH)
        pl.semaphore_wait(barrier, len(partners))

    def send(self, index, slot, partner, source, target):
        copy = pltpu.make_async_remote_copy(
            src_ref=source,
            dst_ref=target,
            send_sem=self.send_sem.at[index, slot],
            recv_sem=self.recv_sem.at[index, slot],
            device_id=partner,
            device_id_type=MESH,
        )
        copy.start()
        self.copies.append(copy)
        return copy

    def halve(self, index, step):
        group, base, size, _ = self.streams[index]
        partner, _, give, half = self.places[index][step]
        source = self.sums[group] if step else self.sources[group]
        arrive = base + size - (size >> step)
        return self.send(
            index, step, partner,
            source.at[pl.ds(give, half)], self.landing[group].at[pl.ds(arrive, half)],
        )

    def add(self, index, step):
        group, base, size, _ = self.streams[index]
        _, keep, _, half = self.places[index][step]
        source = self.sums[group] if step else self.sources[group]
        target = self.sums[group] if step < self.rounds - 1 else self.totals[group]
        landing = self.landing[group]
        arrive = base + size - (size >> step)
        chunk = chunk_of(half)

        def body(i, carry):
            at = pl.ds(keep + i * chunk, chunk)
            target[at] = source[at] + landing[pl.ds(arrive + i * chunk, chunk)]
            return carry

        lax.fori_loop(0, half // chunk, body, 0)

    def double(self, index, step):
        group = self.streams[index][0]
        partner, keep, _, half = self.places[index][step]
        block = self.totals[group].at[pl.ds(keep, half)]
        return self.send(index, 2 * self.rounds - 1 - step, partner, block, block)

    def run(self):
        count = len(self.streams)
        flying = [self.halve(index, 0) for index in range(count)]
        for step in range(self.rounds):
            for index in range(count):
                flying[index].wait_recv()
                self.add(index, step)
                if step < self.rounds - 1:
                    flying[index] = self.halve(index, step + 1)
                else:
                    flying[index] = self.double(index, step)
        for step in reversed(range(self.rounds)):
            for index in range(count):
                flying[index].wait_recv()
                if step:
                    flying[index] = self.double(index, step - 1)
        for copy in self.copies:
            copy.wait_send()


def reduce_kernel(
    streams, ffn_ref, att_ref, ffn_out, att_out, ffn_sum, att_sum, ffn_land, att_land, send_sem, recv_sem
):
    exchange = Exchange(
        streams, (ffn_ref, att_ref), (ffn_sum, att_sum), (ffn_land, att_land), (ffn_out, att_out),
        send_sem, recv_sem,
    )
    exchange.greet()
    exchange.run()


def finish_kernel(ffn_ref, att_ref, gq_ref, gp_ref, g1_ref, g2_ref, table_ref):
    def squares(ref):
        chunk = chunk_of(ref.shape[0])

        def body(i, total):
            block = ref[pl.ds(i * chunk, chunk)].astype(f32)
            return total + jnp.sum(block * block, 0)

        return lax.fori_loop(0, ref.shape[0] // chunk, body, jnp.zeros((SUB, LANE), f32))

    norm_sq = jnp.sum(squares(ffn_ref) + squares(att_ref))
    norm_sq = jnp.full((SUB // 2, LANE), norm_sq, f32)
    factor = jnp.minimum(1.0, math.sqrt(PARAMS) / (jnp.sqrt(norm_sq) + 1e-06))[:1]
    at = 0
    for ref, source in ((g1_ref, ffn_ref), (g2_ref, ffn_ref), (gq_ref, att_ref), (gp_ref, att_ref)):
        at = 0 if ref is gq_ref else at
        rows, lanes = ref.shape
        for column in range(lanes // LANE):
            ref[:, column * LANE : (column + 1) * LANE] = from_tiles(source, at, rows, column) * factor
        at += ref.size // TILE
    for column in range(2):
        table_ref[:, column * LANE : (column + 1) * LANE] = from_tiles(att_ref, at, SUB, column) * factor


def forward_kernel(
    windows, steps, tok_ref, ct_ref, col_ref, row_ref, bias_ref, wq_ref, wp_ref, w1_ref, w2_ref,
    out_ref, mid_ref, qkv_ref, attn_ref, probs_ref, tiles_ref, acc1, acc2,
):
    step = pl.program_id(0)

    @pl.when(step == 0)
    def _():
        acc1[...] = jnp.zeros_like(acc1)
        acc2[...] = jnp.zeros_like(acc2)

    channels = tok_ref.shape[1]
    token = tok_ref[...].astype(f32)
    normal, _ = normalize(token)
    qkv_ref[...] = product(normal.astype(bf16), wq_ref[...], 1, 0).astype(bf16)
    mask = head_mask()
    mask_low = mask.astype(bf16)
    for w in range(windows):
        at = slice(w * SLOTS, (w + 1) * SLOTS)
        same = col_ref[at, :] == row_ref[w]
        hidden = jnp.where(same, 0.0, -1e30)
        hidden = jnp.concatenate([hidden] * GROUP, 0)
        for g in range(GROUPS):
            lanes = g * LANES
            query = stack_heads(qkv_ref[at, lanes : lanes + LANES], mask_low)
            key = qkv_ref[at, channels + lanes : channels + lanes + LANES]
            value = qkv_ref[at, 2 * channels + lanes : 2 * channels + lanes + LANES]
            bias = bias_ref[g * GROUP * SLOTS : (g + 1) * GROUP * SLOTS, :]
            scores = product(query, key, 1, 1) * HEAD_DIM ** (-0.5) + bias + hidden
            exponent = jnp.exp(scores - jnp.max(scores, -1, keepdims=True))
            probs = exponent * (1.0 / jnp.sum(exponent, -1, keepdims=True))
            start = (w * GROUPS + g) * GROUP * SLOTS
            probs_ref[start : start + GROUP * SLOTS, :] = probs
            mixed = product(probs.astype(bf16), value, 1, 0)
            attn_ref[at, lanes : lanes + LANES] = gather_heads(mixed, mask).astype(bf16)
    projected = product(attn_ref[...], wp_ref[...], 1, 0).astype(bf16)
    middle = token + projected.astype(f32)
    second, scale = normalize(middle)
    low = second.astype(bf16)
    upstream = ct_ref[...]
    low_turned = low.T
    up_turned = upstream.T
    hidden_units = w1_ref.shape[1]
    width = hidden_units // FFN_CHUNKS
    total = middle
    back = jnp.zeros_like(middle)
    for c in range(FFN_CHUNKS):
        at = slice(c * width, (c + 1) * width)
        w1 = w1_ref[:, at]
        w2 = w2_ref[at, :]
        pre = product(low, w1, 1, 0)
        cdf = 0.5 * (1.0 + lax.erf(pre * 2.0 ** (-0.5)))
        density = jnp.exp(-0.5 * pre * pre) * (2.0 * math.pi) ** (-0.5)
        active = (pre * cdf).astype(bf16)
        total = total + product(active, w2, 1, 0)
        acc2[:, at] += product(up_turned, active, 1, 0)
        grad_pre = (product(upstream, w2, 1, 1) * (cdf + pre * density)).astype(bf16)
        acc1[:, at] += product(low_turned, grad_pre, 1, 0)
        back = back + product(grad_pre, w1, 1, 1)
    out_ref[...] = total.astype(bf16)
    mid_ref[...] = upstream.astype(f32) + normalize_back(second, scale, back)

    @pl.when(step == steps - 1)
    def _():
        to_tiles(acc1[...], tiles_ref, 0)
        to_tiles(acc2[...].T, tiles_ref, acc1.size // TILE)
        used = (acc1.size + acc2.size) // TILE
        if used < tiles_ref.shape[0]:
            tiles_ref[used:] = jnp.zeros((tiles_ref.shape[0] - used, SUB, LANE), bf16)


def backward_kernel(
    windows, steps, tok_ref, mid_ref, qkv_ref, attn_ref, probs_ref, wq_ref, wp_ref,
    grad_ref, tiles_ref, table_ref, accq, accp, up_ref, gq_ref,
):
    step = pl.program_id(0)

    @pl.when(step == 0)
    def _():
        accq[...] = jnp.zeros_like(accq)
        accp[...] = jnp.zeros_like(accp)
        table_ref[...] = jnp.zeros_like(table_ref)

    channels = tok_ref.shape[1]
    grad_mid = mid_ref[...]
    low = grad_mid.astype(bf16)
    accp[...] += product(attn_ref[...], low, 0, 0)
    up_ref[...] = product(low, wp_ref[...], 1, 1).astype(bf16)
    mask = head_mask()
    mask_low = mask.astype(bf16)
    for w in range(windows):
        at = slice(w * SLOTS, (w + 1) * SLOTS)
        for g in range(GROUPS):
            first = slice(g * LANES, (g + 1) * LANES)
            second = slice(channels + g * LANES, channels + (g + 1) * LANES)
            third = slice(2 * channels + g * LANES, 2 * channels + (g + 1) * LANES)
            rows = slice(g * GROUP * SLOTS, (g + 1) * GROUP * SLOTS)
            query = stack_heads(qkv_ref[at, first], mask_low)
            key = qkv_ref[at, second]
            value = qkv_ref[at, third]
            upstream = stack_heads(up_ref[at, first], mask_low)
            start = (w * GROUPS + g) * GROUP * SLOTS
            probs = probs_ref[start : start + GROUP * SLOTS, :]
            grad_probs = product(upstream, value, 1, 1)
            inner = jnp.sum(probs * grad_probs, -1, keepdims=True)
            grad_scores = probs * (grad_probs - inner)
            table_ref[rows, :] += grad_scores
            scaled = (grad_scores * HEAD_DIM ** (-0.5)).astype(bf16)
            gq_ref[at, first] = gather_heads(product(scaled, key, 1, 0), mask).astype(bf16)
            gq_ref[at, second] = product(scaled, query, 0, 0).astype(bf16)
            gq_ref[at, third] = product(probs.astype(bf16), upstream, 0, 0).astype(bf16)
    normal, scale = normalize(tok_ref[...].astype(f32))
    grads = gq_ref[...]
    accq[...] += product(normal.astype(bf16), grads, 0, 0)
    grad_normed = product(grads, wq_ref[...], 1, 1).astype(bf16).astype(f32)
    grad_ref[...] = (grad_mid + normalize_back(normal, scale, grad_normed)).astype(bf16)

    @pl.when(step == steps - 1)
    def _():
        used = (accq.size + accp.size) // TILE
        to_tiles(accq[...], tiles_ref, 0)
        to_tiles(accp[...], tiles_ref, accq.size // TILE)
        tiles_ref[used:] = jnp.zeros((tiles_ref.shape[0] - used, SUB, LANE), bf16)


def rows_of(shape, at=0):
    return pl.BlockSpec(shape, lambda i: (i, at))


def whole(shape):
    return pl.BlockSpec(shape, lambda i: (0,) * len(shape))


def local(tokens, cotangent, w_qkv, w_proj, w_fc1, w_fc2, bias_table, rel_index, region):
    tile_rows, tile_cols, channels = tokens.shape
    ffn = w_fc1.shape[1]
    count = (tile_rows // SIDE) * (tile_cols // SIDE)
    windows = math.gcd(count, 4)
    steps = count // windows
    block = windows * SLOTS
    total = count * SLOTS

    both = to_shifted(jnp.concatenate([tokens, cotangent], -1))
    cells = to_cells(both, 0)
    region_cells = to_cells(region[..., None], -1)
    region_rows = region_cells.reshape(count, 1, SLOTS)

    extra = CELL - SIDE
    places = jnp.pad(
        rel_index.reshape(SIDE, SIDE, SIDE, SIDE), ((0, extra),) * 4, constant_values=-1
    ).reshape(1, SLOTS * SLOTS)
    lookup = (jnp.arange(TABLE, dtype=jnp.int32)[:, None] == places).astype(f32)
    pos_bias = lax.dot_general(
        bias_table, lookup, (((0,), (0,)), ((), ())), precision=highest
    ).reshape(HEADS * SLOTS, SLOTS)

    across = (lax.axis_size("ha"), lax.axis_size("wa"))
    devices = across[0] * across[1]
    ffn_tiles = 2 * channels * ffn // TILE
    att_used = 4 * channels * channels // TILE
    ffn_padded = padded_tiles(ffn_tiles, devices)
    att_padded = padded_tiles(att_used + 2, devices)

    params = pltpu.CompilerParams(
        dimension_semantics=("arbitrary",), vmem_limit_bytes=60 * 1024 * 1024
    )
    shape = jax.ShapeDtypeStruct
    block_cells, grad_mid, qkv, attn, probs, ffn_grads = pl.pallas_call(
        functools.partial(forward_kernel, windows, steps),
        name="forward",
        grid=(steps,),
        in_specs=[
            rows_of((block, channels)),
            rows_of((block, channels), 1),
            rows_of((block, 1)),
            pl.BlockSpec((windows, 1, SLOTS), lambda i: (i, 0, 0)),
            whole((HEADS * SLOTS, SLOTS)),
            whole((channels, 3 * channels)),
            whole((channels, channels)),
            whole((channels, ffn)),
            whole((ffn, channels)),
        ],
        out_specs=[
            rows_of((block, channels)),
            rows_of((block, channels)),
            rows_of((block, 3 * channels)),
            rows_of((block, channels)),
            rows_of((windows * HEADS * SLOTS, SLOTS)),
            whole((ffn_padded, SUB, LANE)),
        ],
        out_shape=[
            shape((total, channels), bf16),
            shape((total, channels), f32),
            shape((total, 3 * channels), bf16),
            shape((total, channels), bf16),
            shape((count * HEADS * SLOTS, SLOTS), f32),
            shape((ffn_padded, SUB, LANE), bf16),
        ],
        scratch_shapes=[pltpu.VMEM((channels, ffn), f32), pltpu.VMEM((channels, ffn), f32)],
        compiler_params=params,
        cost_estimate=pl.CostEstimate(
            flops=20_000_000_000, bytes_accessed=20_000_000, transcendentals=4_000_000
        ),
    )(cells, cells, region_cells, region_rows, pos_bias, w_qkv, w_proj, w_fc1, w_fc2)
    block_out = from_shifted(from_cells(block_cells, tile_rows, tile_cols))

    grad_cells, att_grads, bias_grad = pl.pallas_call(
        functools.partial(backward_kernel, windows, steps),
        name="backward",
        grid=(steps,),
        in_specs=[
            rows_of((block, channels)),
            rows_of((block, channels)),
            rows_of((block, 3 * channels)),
            rows_of((block, channels)),
            rows_of((windows * HEADS * SLOTS, SLOTS)),
            whole((channels, 3 * channels)),
            whole((channels, channels)),
        ],
        out_specs=[
            rows_of((block, channels)),
            whole((att_padded, SUB, LANE)),
            whole((HEADS * SLOTS, SLOTS)),
        ],
        out_shape=[
            shape((total, channels), bf16),
            shape((att_padded, SUB, LANE), bf16),
            shape((HEADS * SLOTS, SLOTS), f32),
        ],
        scratch_shapes=[
            pltpu.VMEM((channels, 3 * channels), f32),
            pltpu.VMEM((channels, channels), f32),
            pltpu.VMEM((block, channels), bf16),
            pltpu.VMEM((block, 3 * channels), bf16),
        ],
        compiler_params=params,
        cost_estimate=pl.CostEstimate(
            flops=16_000_000_000, bytes_accessed=16_000_000, transcendentals=1_000_000
        ),
    )(cells, grad_mid, qkv, attn, probs, w_qkv, w_proj)
    grad_table = lax.dot_general(
        bias_grad.reshape(HEADS, SLOTS * SLOTS), lookup, (((1,), (1,)), ((), ())), precision=highest
    )
    table_tiles = jnp.pad(grad_table, ((0, SUB - HEADS), (0, 2 * LANE - TABLE))).astype(bf16)
    table_tiles = table_tiles.reshape(SUB, 2, LANE).transpose(1, 0, 2)
    att_grads = lax.dynamic_update_slice(att_grads, table_tiles, (att_used, 0, 0))

    orders = link_orders(*across)
    streams = split_streams(0, ffn_padded, devices, STREAMS[0], orders)
    streams += split_streams(1, att_padded, devices, STREAMS[1], orders)
    tiled = (shape((ffn_padded, SUB, LANE), bf16), shape((att_padded, SUB, LANE), bf16))
    in_vmem = pl.BlockSpec(memory_space=pltpu.VMEM)
    semaphores = pltpu.SemaphoreType.DMA((len(streams), 2 * len(orders[0])))
    ffn_sum, att_sum = pl.pallas_call(
        functools.partial(reduce_kernel, streams),
        name="reduce",
        out_shape=tiled,
        in_specs=[in_vmem] * 2,
        out_specs=[in_vmem] * 2,
        scratch_shapes=[pltpu.VMEM(part.shape, bf16) for part in tiled] * 2 + [semaphores] * 2,
        compiler_params=pltpu.CompilerParams(
            collective_id=0, has_side_effects=True, vmem_limit_bytes=60 * 1024 * 1024
        ),
    )(ffn_grads, att_grads)
    token_grad = from_shifted(from_cells(grad_cells, tile_rows, tile_cols))

    gq, gp, g1, g2, table = pl.pallas_call(
        finish_kernel,
        name="finish",
        out_shape=[
            shape((channels, 3 * channels), f32),
            shape((channels, channels), f32),
            shape((channels, ffn), f32),
            shape((ffn, channels), f32),
            shape((SUB, 2 * LANE), f32),
        ],
        in_specs=[in_vmem] * 2,
        out_specs=[in_vmem] * 5,
        compiler_params=pltpu.CompilerParams(vmem_limit_bytes=60 * 1024 * 1024),
    )(ffn_sum, att_sum)
    return (block_out, token_grad, gq, gp, g1, g2, table[:HEADS, :TABLE].T)


def solution(mesh):
    placed = (P("ha", "wa", None), P("ha", "wa", None), P(), P(), P(), P(), P(), P(), P("ha", "wa"))
    return jax.shard_map(
        local,
        mesh=mesh,
        in_specs=placed,
        out_specs=(P("ha", "wa", None), P("ha", "wa", None), P(), P(), P(), P(), P()),
        check_vma=False,
    )
```

```python
import functools
import math

import jax
import jax.numpy as jnp
from jax import lax
from jax.experimental import pallas as pl
from jax.experimental.pallas import tpu as pltpu
from jax.sharding import PartitionSpec as P

HEADS = 12
SIDE = 7
SHIFT = 3
HEAD_DIM = 32
TABLE = 169
PARAMS = 1771500
CELL = 8
SLOTS = CELL * CELL
GROUP = 4
LANES = GROUP * HEAD_DIM
GROUPS = HEADS // GROUP
FFN_CHUNKS = 3
SUB = 16
LANE = 128
TILE = SUB * LANE
STREAMS = (4, 2)
PAIR = 2
SLOT_MOVES = ((), (0, 1, 2, 3), (), (0, 1), (2, 3), (0, 1), (2, 3, 0, 1), (2, 3))
MESH = pl.DeviceIdType.MESH

epsilon = 1e-05
highest = lax.Precision.HIGHEST
f32 = jnp.float32
bf16 = jnp.bfloat16


def from_behind(x, axis, by):
    count = lax.axis_size(axis)
    return lax.ppermute(x, axis, [(i, (i + by) % count) for i in range(count)])


def to_shifted(grid_in):
    lower_rim = from_behind(grid_in[:SHIFT], "ha", -1)
    taller = jnp.concatenate([grid_in[SHIFT:], lower_rim], 0)
    right_rim = from_behind(taller[:, :SHIFT], "wa", -1)
    return jnp.concatenate([taller[:, SHIFT:], right_rim], 1)


def from_shifted(grid_in):
    upper_rim = from_behind(grid_in[-SHIFT:], "ha", 1)
    taller = jnp.concatenate([upper_rim, grid_in[:-SHIFT]], 0)
    left_rim = from_behind(taller[:, -SHIFT:], "wa", 1)
    return jnp.concatenate([left_rim, taller[:, :-SHIFT]], 1)


def to_cells(grid_in, fill):
    rows, cols, channels = grid_in.shape
    split = grid_in.reshape(rows // SIDE, SIDE, cols // SIDE, SIDE, channels)
    extra = CELL - SIDE
    padded = jnp.pad(
        split, ((0, 0), (0, extra), (0, 0), (0, extra), (0, 0)), constant_values=fill
    )
    return padded.transpose(0, 2, 1, 3, 4).reshape(-1, channels)


def from_cells(flat, rows, cols):
    split = flat.reshape(rows // SIDE, cols // SIDE, CELL, CELL, -1)[:, :, :SIDE, :SIDE]
    return split.transpose(0, 2, 1, 3, 4).reshape(rows, cols, -1)


def normalize(values):
    average = jnp.mean(values, -1, keepdims=True)
    centred = values - average
    inverse = lax.rsqrt(jnp.mean(centred * centred, -1, keepdims=True) + epsilon)
    return (centred * inverse, inverse)


def normalize_back(normal_rows, inverse, upstream):
    up_mean = jnp.mean(upstream, -1, keepdims=True)
    cross_mean = jnp.mean(upstream * normal_rows, -1, keepdims=True)
    return inverse * (upstream - up_mean - normal_rows * cross_mean)


def product(left, right, left_dim, right_dim):
    return lax.dot_general(
        left, right, (((left_dim,), (right_dim,)), ((), ())), preferred_element_type=f32
    )


def head_mask():
    shape = (GROUP * SLOTS, LANES)
    row_head = lax.broadcasted_iota(jnp.int32, shape, 0) // SLOTS
    lane_head = lax.broadcasted_iota(jnp.int32, shape, 1) // HEAD_DIM
    return (row_head == lane_head).astype(f32)


def stack_heads(rows, mask):
    return jnp.concatenate([rows] * GROUP, 0) * mask


def gather_heads(stacked, mask):
    kept = stacked * mask
    total = kept[:SLOTS]
    for head in range(1, GROUP):
        total = total + kept[head * SLOTS : (head + 1) * SLOTS]
    return total


def to_tiles(values, tiles_ref, at):
    rows, lanes = values.shape
    high = rows // SUB
    low = values.astype(bf16)
    for column in range(lanes // LANE):
        block = low[:, column * LANE : (column + 1) * LANE].reshape(high, SUB, LANE)
        tiles_ref[at + column * high : at + (column + 1) * high] = block


def from_tiles(tiles_ref, at, rows, column):
    high = rows // SUB
    block = tiles_ref[at + column * high : at + (column + 1) * high]
    return block.reshape(rows, LANE).astype(f32)


def strides_of(size):
    return [1 << i for i in range(size.bit_length() - 1)]


def link_orders(across_ha, across_wa):
    first, *far = [("wa", stride) for stride in strides_of(across_wa)]
    near = [("ha", stride) for stride in strides_of(across_ha)]
    return ([first] + near + far, [first] + near[::-1] + far)


def split_streams(group, tiles, devices, parts, orders):
    units = tiles // devices
    streams = []
    base = 0
    for part in range(parts):
        size = (units // parts + (part < units % parts)) * devices
        if size:
            streams.append((group, base, size, orders[part % len(orders)]))
        base += size
    return streams


def padded_tiles(tiles, devices):
    return -(-tiles // devices) * devices


def chunk_of(count):
    return max(size for size in range(1, 17) if count % size == 0)


class Exchange:
    def __init__(self, streams, sources, sums, landing, totals, send_sem, recv_sem):
        self.streams = streams
        self.sources, self.sums, self.landing, self.totals = sources, sums, landing, totals
        self.send_sem, self.recv_sem = send_sem, recv_sem
        self.rounds = len(streams[0][3])
        self.done = [0] * len(streams)
        self.places = []
        for group, base, size, order in streams:
            places = []
            low = base
            for step, (axis, stride) in enumerate(order):
                half = size >> (step + 1)
                me = lax.axis_index(axis)
                bit = (me // stride) % 2
                partner = {axis: me + stride - 2 * stride * bit}
                keep = low + bit * half
                give = low + half - bit * half
                places.append((partner, keep, give, half))
                low = keep
            self.places.append(places)
        self.partners = {
            link: place[0]
            for stream, places in zip(streams, self.places)
            for link, place in zip(stream[3], places)
        }

    def greet(self):
        barrier = pltpu.get_barrier_semaphore()
        for partner in self.partners.values():
            pl.semaphore_signal(barrier, inc=1, device_id=partner, device_id_type=MESH)

    def meet(self):
        pl.semaphore_wait(pltpu.get_barrier_semaphore(), len(self.partners))

    def arrival(self, index, step):
        _, base, size, _ = self.streams[index]
        return base + size - (size >> step)

    def copy(self, index, slot):
        group = self.streams[index][0]
        if slot < self.rounds:
            partner, _, give, half = self.places[index][slot]
            source = (self.sums if slot else self.sources)[group].at[pl.ds(give, half)]
            target = self.landing[group].at[pl.ds(self.arrival(index, slot), half)]
        else:
            partner, keep, _, half = self.places[index][2 * self.rounds - 1 - slot]
            source = self.totals[group].at[pl.ds(keep, half)]
            target = source
        return pltpu.make_async_remote_copy(
            src_ref=source,
            dst_ref=target,
            send_sem=self.send_sem.at[index, slot],
            recv_sem=self.recv_sem.at[index, slot],
            device_id=partner,
            device_id_type=MESH,
        )

    def add(self, index, step):
        group = self.streams[index][0]
        _, keep, _, half = self.places[index][step]
        source = (self.sums if step else self.sources)[group]
        target = (self.sums if step < self.rounds - 1 else self.totals)[group]
        landing = self.landing[group]
        arrive = self.arrival(index, step)
        chunk = chunk_of(half)

        def body(i, carry):
            at = pl.ds(keep + i * chunk, chunk)
            target[at] = source[at] + landing[pl.ds(arrive + i * chunk, chunk)]
            return carry

        lax.fori_loop(0, half // chunk, body, 0)

    def start(self, index):
        self.copy(index, 0).start()

    def advance(self, index):
        slot = self.done[index]
        if slot == 2 * self.rounds:
            return
        self.copy(index, slot).wait_recv()
        if slot < self.rounds:
            self.add(index, slot)
        if slot + 1 < 2 * self.rounds:
            self.copy(index, slot + 1).start()
        self.done[index] = slot + 1

    def drain(self, order):
        while any(self.done[index] < 2 * self.rounds for index in order):
            for index in order:
                self.advance(index)

    def close(self):
        for index in range(len(self.streams)):
            for slot in range(2 * self.rounds):
                self.copy(index, slot).wait_send()


def picks(offset_ref, place):
    labels = lax.broadcasted_iota(jnp.int32, (2 * LANE, LANE), 0)
    return (labels == offset_ref[place : place + 1, :]).astype(f32).astype(bf16)


def fill_bias(offset_ref, label_ref, spread_ref, bias_ref):
    rest = label_ref[...]
    parts = []
    for _ in range(3):
        part = rest.astype(bf16)
        parts.append(part)
        rest = rest - part.astype(f32)
    parts = jnp.concatenate(parts, 0)
    for place in range(CELL):
        spread = product(parts, picks(offset_ref, place), 1, 0)
        spread = spread[:SUB] + (spread[SUB : 2 * SUB] + spread[2 * SUB :])
        spread_ref[pl.ds(place, HEADS, stride=CELL), :] = spread[:HEADS]
    for head in range(HEADS):
        rows = spread_ref[head * CELL : (head + 1) * CELL, :]
        for row in range(CELL):
            at = head * SLOTS + row * CELL
            if row < SIDE:
                turned = pltpu.roll(rows, LANE - (SIDE - row) * CELL, 1)
                bias_ref[at : at + CELL, :] = turned[:, :SLOTS]
            else:
                bias_ref[at : at + CELL, :] = jnp.zeros((CELL, SLOTS), f32)


def gather_offsets(scores_ref, spread_ref, tiles_ref, first):
    for head in range(HEADS):
        total = jnp.zeros((CELL, LANE), f32)
        for row in range(SIDE):
            at = head * SLOTS + row * CELL
            total = total + pltpu.roll(scores_ref[at : at + CELL, :], (SIDE - row) * CELL, 1)
        spread_ref[head * CELL : (head + 1) * CELL, :] = total
    for place in range(CELL):
        rows = spread_ref[pl.ds(place, HEADS, stride=CELL), :]
        rows = jnp.concatenate([rows, jnp.zeros((SUB - HEADS, LANE), f32)], 0)
        tiles_ref[first + place] = rows.astype(bf16)


def block_kernel(
    windows, streams, slots,
    cell_ref, region_ref, offset_ref, label_ref, wq_ref, wp_ref, w1_ref, w2_ref,
    out_ref, grad_ref, early_out, late_out,
    bias_ref, spread_ref, scores_ref, normal_ref, qkv_ref, attn_ref, probs_ref, mid_ref, up_ref, gq_ref,
    acc1, acc2, early_in, late_in, early_sum, late_sum, early_land, late_land, send_sem, recv_sem,
):
    exchange = Exchange(
        streams, (early_in, late_in), (early_sum, late_sum), (early_land, late_land), (early_out, late_out),
        send_sem, recv_sem,
    )
    early = [index for index, stream in enumerate(streams) if stream[0] == 0]
    late = [index for index, stream in enumerate(streams) if stream[0] == 1]
    exchange.greet()
    total_rows, channels = out_ref.shape
    count = total_rows // SLOTS
    block = windows * SLOTS
    hidden_units = w1_ref.shape[1]
    width = hidden_units // FFN_CHUNKS
    stacked_rows = GROUP * SLOTS
    mask = head_mask()
    mask_low = mask.astype(bf16)
    fill_bias(offset_ref, label_ref, spread_ref, bias_ref)
    acc1[...] = jnp.zeros_like(acc1)
    acc2[...] = jnp.zeros_like(acc2)

    def forward(step, carry):
        rows = pl.ds(pl.multiple_of(step * block, block), block)
        token = cell_ref[rows, :channels].astype(f32)
        upstream = cell_ref[rows, channels:]
        normal, _ = normalize(token)
        normal_low = normal.astype(bf16)
        normal_ref[rows, :] = normal_low
        qkv_ref[rows, :] = product(normal_low, wq_ref[...], 1, 0).astype(bf16)
        for w in range(windows):
            at = pl.ds(pl.multiple_of(step * block + w * SLOTS, SLOTS), SLOTS)
            labels = jnp.broadcast_to(region_ref[step * windows + w], (SLOTS, SLOTS))
            hidden = jnp.where(labels == labels.T, 0.0, -1e30)
            hidden = jnp.concatenate([hidden] * GROUP, 0)
            for g in range(GROUPS):
                lanes = g * LANES
                query = stack_heads(qkv_ref[at, lanes : lanes + LANES], mask_low)
                key = qkv_ref[at, channels + lanes : channels + lanes + LANES]
                value = qkv_ref[at, 2 * channels + lanes : 2 * channels + lanes + LANES]
                bias = bias_ref[g * stacked_rows : (g + 1) * stacked_rows, :]
                scores = product(query, key, 1, 1) * HEAD_DIM ** (-0.5) + bias + hidden
                exponent = jnp.exp(scores - jnp.max(scores, -1, keepdims=True))
                probs = (exponent * (1.0 / jnp.sum(exponent, -1, keepdims=True))).astype(bf16)
                start = ((step * windows + w) * GROUPS + g) * stacked_rows
                probs_ref[pl.ds(pl.multiple_of(start, stacked_rows), stacked_rows), :] = probs
                mixed = product(probs, value, 1, 0)
                attn_ref[at, lanes : lanes + LANES] = gather_heads(mixed, mask).astype(bf16)
        projected = product(attn_ref[rows, :], wp_ref[...], 1, 0).astype(bf16)
        middle = token + projected.astype(f32)
        second, scale = normalize(middle)
        low = second.astype(bf16)
        low_turned = low.T
        up_turned = upstream.T
        total = middle
        back = jnp.zeros_like(middle)
        for c in range(FFN_CHUNKS):
            at = slice(c * width, (c + 1) * width)
            w1 = w1_ref[:, at]
            w2 = w2_ref[at, :]
            pre = product(low, w1, 1, 0)
            cdf = 0.5 * (1.0 + lax.erf(pre * 2.0 ** (-0.5)))
            density = jnp.exp(-0.5 * pre * pre) * (2.0 * math.pi) ** (-0.5)
            active = (pre * cdf).astype(bf16)
            total = total + product(active, w2, 1, 0)
            acc2[:, at] += product(up_turned, active, 1, 0)
            grad_pre = (product(upstream, w2, 1, 1) * (cdf + pre * density)).astype(bf16)
            acc1[:, at] += product(low_turned, grad_pre, 1, 0)
            back = back + product(grad_pre, w1, 1, 1)
        out_ref[rows, :] = total.astype(bf16)
        mid_ref[rows, :] = upstream.astype(f32) + normalize_back(second, scale, back)
        return carry

    lax.fori_loop(0, count // windows, forward, 0)

    mid_low = mid_ref[...].astype(bf16)
    to_tiles(acc1[...], early_in, 0)
    to_tiles(acc2[...].T, early_in, acc1.size // TILE)
    used = 2 * acc1.size // TILE
    to_tiles(product(attn_ref[...], mid_low, 0, 0), early_in, used)
    used += channels * channels // TILE
    if used < early_in.shape[0]:
        early_in[used:] = jnp.zeros((early_in.shape[0] - used, SUB, LANE), bf16)
    exchange.meet()
    for index in early:
        exchange.start(index)
    up_ref[...] = product(mid_low, wp_ref[...], 1, 1).astype(bf16)
    scores_ref[...] = jnp.zeros_like(scores_ref)

    def backward(step, carry):
        for slot, moves in enumerate(slots):
            if moves:
                @pl.when(step == slot)
                def _(moves=moves):
                    for index in moves:
                        exchange.advance(index)

        for w in range(PAIR):
            at = pl.ds(pl.multiple_of((step * PAIR + w) * SLOTS, SLOTS), SLOTS)
            for g in range(GROUPS):
                first = slice(g * LANES, (g + 1) * LANES)
                second = slice(channels + g * LANES, channels + (g + 1) * LANES)
                third = slice(2 * channels + g * LANES, 2 * channels + (g + 1) * LANES)
                rows = slice(g * stacked_rows, (g + 1) * stacked_rows)
                query = stack_heads(qkv_ref[at, first], mask_low)
                key = qkv_ref[at, second]
                value = qkv_ref[at, third]
                upstream = stack_heads(up_ref[at, first], mask_low)
                start = ((step * PAIR + w) * GROUPS + g) * stacked_rows
                low = probs_ref[pl.ds(pl.multiple_of(start, stacked_rows), stacked_rows), :]
                probs = low.astype(f32)
                grad_probs = product(upstream, value, 1, 1)
                inner = jnp.sum(probs * grad_probs, -1, keepdims=True)
                grad_scores = probs * (grad_probs - inner)
                scores_ref[rows, :SLOTS] += grad_scores
                scaled = (grad_scores * HEAD_DIM ** (-0.5)).astype(bf16)
                gq_ref[at, first] = gather_heads(product(scaled, key, 1, 0), mask).astype(bf16)
                gq_ref[at, second] = product(scaled, query, 0, 0).astype(bf16)
                gq_ref[at, third] = product(low, upstream, 0, 0).astype(bf16)
        return carry

    lax.fori_loop(0, count // PAIR, backward, 0)

    normal_turned = normal_ref[...].T
    to_tiles(product(normal_turned, gq_ref[...], 1, 0), late_in, 0)
    used = 3 * channels * channels // TILE
    gather_offsets(scores_ref, spread_ref, late_in, used)
    used += CELL
    if used < late_in.shape[0]:
        late_in[used:] = jnp.zeros((late_in.shape[0] - used, SUB, LANE), bf16)
    for index in late:
        exchange.start(index)

    def finish_tokens(step, carry):
        rows = pl.ds(pl.multiple_of(step * block, block), block)
        normal, scale = normalize(cell_ref[rows, :channels].astype(f32))
        grad_normed = product(gq_ref[rows, :], wq_ref[...], 1, 1).astype(bf16).astype(f32)
        grad_ref[rows, :] = (mid_ref[rows, :] + normalize_back(normal, scale, grad_normed)).astype(bf16)
        return carry

    lax.fori_loop(0, count // windows, finish_tokens, 0)
    exchange.drain(late + early)
    exchange.close()


def finish_kernel(early_ref, late_ref, offset_ref, gq_ref, gp_ref, g1_ref, g2_ref, table_ref):
    def squares(ref, first, last):
        chunk = chunk_of(last - first)

        def body(i, total):
            block = ref[pl.ds(first + i * chunk, chunk)].astype(f32)
            return total + jnp.sum(block * block, 0)

        return lax.fori_loop(0, (last - first) // chunk, body, jnp.zeros((SUB, LANE), f32))

    used = gq_ref.size // TILE
    table = jnp.zeros((SUB, 2 * LANE), f32)
    for place in range(CELL):
        table = table + product(late_ref[used + place], picks(offset_ref, place), 1, 1)
    norm_sq = jnp.sum(squares(early_ref, 0, early_ref.shape[0]) + squares(late_ref, 0, used))
    norm_sq = norm_sq + jnp.sum(table * table)
    norm_sq = jnp.full((SUB // 2, LANE), norm_sq, f32)
    factor = jnp.minimum(1.0, math.sqrt(PARAMS) / (jnp.sqrt(norm_sq) + 1e-06))[:1]
    at = 0
    for ref, source in ((g1_ref, early_ref), (g2_ref, early_ref), (gp_ref, early_ref), (gq_ref, late_ref)):
        at = 0 if ref is gq_ref else at
        rows, lanes = ref.shape
        for column in range(lanes // LANE):
            ref[:, column * LANE : (column + 1) * LANE] = from_tiles(source, at, rows, column) * factor
        at += ref.size // TILE
    for column in range(2):
        lanes = slice(column * LANE, (column + 1) * LANE)
        table_ref[:, lanes] = table[:, lanes] * factor


def offsets_of(rel_index):
    rel = rel_index.reshape(SIDE, SIDE, SIDE, SIDE)
    behind = rel[1:, :, 0][::-1]
    ahead = rel[0].transpose(1, 0, 2)
    places = jnp.concatenate([behind, ahead], 0).transpose(1, 0, 2)
    places = jnp.pad(places, ((0, 1), (1, 2), (0, 1)), constant_values=-1)
    return places.reshape(CELL, LANE)


def local(tokens, cotangent, w_qkv, w_proj, w_fc1, w_fc2, bias_table, rel_index, region):
    tile_rows, tile_cols, channels = tokens.shape
    ffn = w_fc1.shape[1]
    count = (tile_rows // SIDE) * (tile_cols // SIDE)
    windows = math.gcd(count, 4)
    total = count * SLOTS

    both = to_shifted(jnp.concatenate([tokens, cotangent], -1))
    cells = to_cells(both, 0)
    labels = to_cells(region[..., None], -1).astype(f32).reshape(count, 1, SLOTS)
    offsets = offsets_of(rel_index)
    label_rows = jnp.pad(bias_table.T, ((0, SUB - HEADS), (0, 2 * LANE - TABLE)))

    across = (lax.axis_size("ha"), lax.axis_size("wa"))
    devices = across[0] * across[1]
    early_tiles = padded_tiles((2 * channels * ffn + channels * channels) // TILE, devices)
    late_tiles = padded_tiles(3 * channels * channels // TILE + CELL, devices)
    orders = link_orders(*across)
    streams = split_streams(0, early_tiles, devices, STREAMS[0], orders)
    early_count = len(streams)
    streams += split_streams(1, late_tiles, devices, STREAMS[1], orders)
    slots = [[index for index in moves if index < early_count] for moves in SLOT_MOVES[: count // PAIR]]

    shape = jax.ShapeDtypeStruct
    early = (early_tiles, SUB, LANE)
    late = (late_tiles, SUB, LANE)
    in_vmem = pl.BlockSpec(memory_space=pltpu.VMEM)
    semaphores = pltpu.SemaphoreType.DMA((len(streams), 2 * len(orders[0])))
    vmem_limit = 62 * 1024 * 1024
    block_cells, grad_cells, early_sum, late_sum = pl.pallas_call(
        functools.partial(block_kernel, windows, streams, slots),
        name="block",
        out_shape=[
            shape((total, channels), bf16), shape((total, channels), bf16), shape(early, bf16), shape(late, bf16),
        ],
        in_specs=[in_vmem] * 8,
        out_specs=[in_vmem] * 4,
        scratch_shapes=[
            pltpu.VMEM((HEADS * SLOTS, SLOTS), f32),
            pltpu.VMEM((HEADS * CELL, LANE), f32),
            pltpu.VMEM((HEADS * SLOTS, LANE), f32),
            pltpu.VMEM((total, channels), bf16),
            pltpu.VMEM((total, 3 * channels), bf16),
            pltpu.VMEM((total, channels), bf16),
            pltpu.VMEM((count * HEADS * SLOTS, SLOTS), bf16),
            pltpu.VMEM((total, channels), f32),
            pltpu.VMEM((total, channels), bf16),
            pltpu.VMEM((total, 3 * channels), bf16),
            pltpu.VMEM((channels, ffn), f32),
            pltpu.VMEM((channels, ffn), f32),
        ] + [pltpu.VMEM(group, bf16) for group in (early, late)] * 3 + [semaphores] * 2,
        compiler_params=pltpu.CompilerParams(
            collective_id=0, has_side_effects=True, vmem_limit_bytes=vmem_limit
        ),
        cost_estimate=pl.CostEstimate(
            flops=36_000_000_000, bytes_accessed=20_000_000, transcendentals=5_000_000
        ),
    )(cells, labels, offsets, label_rows, w_qkv, w_proj, w_fc1, w_fc2)
    block_out = from_shifted(from_cells(block_cells, tile_rows, tile_cols))
    token_grad = from_shifted(from_cells(grad_cells, tile_rows, tile_cols))

    gq, gp, g1, g2, table = pl.pallas_call(
        finish_kernel,
        name="finish",
        out_shape=[
            shape((channels, 3 * channels), f32),
            shape((channels, channels), f32),
            shape((channels, ffn), f32),
            shape((ffn, channels), f32),
            shape((SUB, 2 * LANE), f32),
        ],
        in_specs=[in_vmem] * 3,
        out_specs=[in_vmem] * 5,
        compiler_params=pltpu.CompilerParams(vmem_limit_bytes=vmem_limit),
    )(early_sum, late_sum, offsets)
    return (block_out, token_grad, gq, gp, g1, g2, table[:HEADS, :TABLE].T)


def solution(mesh):
    placed = (P("ha", "wa", None), P("ha", "wa", None), P(), P(), P(), P(), P(), P(), P("ha", "wa"))
    return jax.shard_map(
        local,
        mesh=mesh,
        in_specs=placed,
        out_specs=(P("ha", "wa", None), P("ha", "wa", None), P(), P(), P(), P(), P()),
        check_vma=False,
    )
```

```python
import functools
import math

import jax
import jax.numpy as jnp
from jax import lax
from jax.experimental import pallas as pl
from jax.experimental.pallas import tpu as pltpu
from jax.sharding import PartitionSpec as P

HEADS = 12
SIDE = 7
SHIFT = 3
HEAD_DIM = 32
TABLE = 169
PARAMS = 1771500
CELL = 8
SLOTS = CELL * CELL
GROUP = 4
LANES = GROUP * HEAD_DIM
GROUPS = HEADS // GROUP
FFN_CHUNKS = 3
SUB = 16
LANE = 128
TILE = SUB * LANE
STREAMS = (4, 2)
PAIR = 2
SLOT_MOVES = ((), (0, 1, 2, 3), (), (0, 1), (2, 3), (0, 1), (2, 3, 0, 1), (2, 3))
MESH = pl.DeviceIdType.MESH
PITCH = 32

epsilon = 1e-05
highest = lax.Precision.HIGHEST
f32 = jnp.float32
bf16 = jnp.bfloat16


def normalize(values):
    average = jnp.mean(values, -1, keepdims=True)
    centred = values - average
    inverse = lax.rsqrt(jnp.mean(centred * centred, -1, keepdims=True) + epsilon)
    return (centred * inverse, inverse)


def normalize_back(normal_rows, inverse, upstream):
    up_mean = jnp.mean(upstream, -1, keepdims=True)
    cross_mean = jnp.mean(upstream * normal_rows, -1, keepdims=True)
    return inverse * (upstream - up_mean - normal_rows * cross_mean)


def product(left, right, left_dim, right_dim):
    return lax.dot_general(
        left, right, (((left_dim,), (right_dim,)), ((), ())), preferred_element_type=f32
    )


def head_mask():
    shape = (GROUP * SLOTS, LANES)
    row_head = lax.broadcasted_iota(jnp.int32, shape, 0) // SLOTS
    lane_head = lax.broadcasted_iota(jnp.int32, shape, 1) // HEAD_DIM
    return (row_head == lane_head).astype(f32)


def stack_heads(rows, mask):
    return jnp.concatenate([rows] * GROUP, 0) * mask


def gather_heads(stacked, mask):
    kept = stacked * mask
    total = kept[:SLOTS]
    for head in range(1, GROUP):
        total = total + kept[head * SLOTS : (head + 1) * SLOTS]
    return total


def to_tiles(values, tiles_ref, at):
    rows, lanes = values.shape
    high = rows // SUB
    low = values.astype(bf16)
    for column in range(lanes // LANE):
        block = low[:, column * LANE : (column + 1) * LANE].reshape(high, SUB, LANE)
        tiles_ref[at + column * high : at + (column + 1) * high] = block


def strides_of(size):
    return [1 << i for i in range(size.bit_length() - 1)]


def link_orders(across_ha, across_wa):
    first, *far = [("wa", stride) for stride in strides_of(across_wa)]
    near = [("ha", stride) for stride in strides_of(across_ha)]
    return ([first] + near + far, [first] + near[::-1] + far)


def split_streams(group, tiles, devices, parts, orders):
    units = tiles // devices
    streams = []
    base = 0
    for part in range(parts):
        size = (units // parts + (part < units % parts)) * devices
        if size:
            streams.append((group, base, size, orders[part % len(orders)]))
        base += size
    return streams


def padded_tiles(tiles, devices):
    return -(-tiles // devices) * devices


def chunk_of(count):
    return max(size for size in range(1, 17) if count % size == 0)


class Exchange:
    def __init__(self, streams, sources, sums, landing, totals, send_sem, recv_sem, limits, square_ref):
        self.streams = streams
        self.sources, self.sums, self.landing, self.totals = sources, sums, landing, totals
        self.send_sem, self.recv_sem = send_sem, recv_sem
        self.limits, self.square_ref = limits, square_ref
        self.rounds = len(streams[0][3])
        self.done = [0] * len(streams)
        self.places = []
        for group, base, size, order in streams:
            places = []
            low = base
            for step, (axis, stride) in enumerate(order):
                half = size >> (step + 1)
                me = lax.axis_index(axis)
                bit = (me // stride) % 2
                partner = {axis: me + stride - 2 * stride * bit}
                keep = low + bit * half
                give = low + half - bit * half
                places.append((partner, keep, give, half))
                low = keep
            self.places.append(places)
        self.partners = {
            link: place[0]
            for stream, places in zip(streams, self.places)
            for link, place in zip(stream[3], places)
        }

    def arrival(self, index, step):
        _, base, size, _ = self.streams[index]
        return base + size - (size >> step)

    def copy(self, index, slot):
        group = self.streams[index][0]
        if slot < self.rounds:
            partner, _, give, half = self.places[index][slot]
            source = (self.sums if slot else self.sources)[group].at[pl.ds(give, half)]
            target = self.landing[group].at[pl.ds(self.arrival(index, slot), half)]
        else:
            partner, keep, _, half = self.places[index][2 * self.rounds - 1 - slot]
            source = self.totals[group].at[pl.ds(keep, half)]
            target = source
        return pltpu.make_async_remote_copy(
            src_ref=source,
            dst_ref=target,
            send_sem=self.send_sem.at[index, slot],
            recv_sem=self.recv_sem.at[index, slot],
            device_id=partner,
            device_id_type=MESH,
        )

    def add(self, index, step):
        group = self.streams[index][0]
        _, keep, _, half = self.places[index][step]
        source = (self.sums if step else self.sources)[group]
        target = (self.sums if step < self.rounds - 1 else self.totals)[group]
        landing = self.landing[group]
        arrive = self.arrival(index, step)
        chunk = chunk_of(half)

        def body(i, carry):
            at = pl.ds(keep + i * chunk, chunk)
            target[at] = source[at] + landing[pl.ds(arrive + i * chunk, chunk)]
            return carry

        lax.fori_loop(0, half // chunk, body, 0)

    def start(self, index):
        self.copy(index, 0).start()

    def advance(self, index):
        slot = self.done[index]
        if slot == 2 * self.rounds:
            return
        self.copy(index, slot).wait_recv()
        if slot < self.rounds:
            self.add(index, slot)
        if slot + 1 < 2 * self.rounds:
            self.copy(index, slot + 1).start()
        if slot == self.rounds - 1:
            _, keep, _, half = self.places[index][slot]
            self.square(index, keep, half)
        elif slot >= self.rounds:
            _, _, give, half = self.places[index][2 * self.rounds - 1 - slot]
            self.square(index, give, half)
        self.done[index] = slot + 1

    def square(self, index, first, length):
        group = self.streams[index][0]
        totals = self.totals[group]
        chunk = chunk_of(length)

        def body(i, total):
            at = first + i * chunk
            block = totals[pl.ds(at, chunk)].astype(f32)
            inside = lax.broadcasted_iota(jnp.int32, block.shape, 0) + at < self.limits[group]
            return total + jnp.sum(jnp.where(inside, block * block, 0.0), 0)

        total = lax.fori_loop(0, length // chunk, body, jnp.zeros((SUB, LANE), f32))
        self.square_ref[...] += total

    def drain(self, order):
        while any(self.done[index] < 2 * self.rounds for index in order):
            for index in order:
                self.advance(index)

    def close(self):
        for index in range(len(self.streams)):
            for slot in range(2 * self.rounds):
                self.copy(index, slot).wait_send()


class Rims:
    def __init__(self, by, send_sem, recv_sem, phase):
        spots = {}
        for axis in ("ha", "wa"):
            count = lax.axis_size(axis)
            spots[axis] = (lax.axis_index(axis) + by + count) % count
        self.targets = ({"ha": spots["ha"]}, {"wa": spots["wa"]}, spots)
        self.send_sem, self.recv_sem, self.phase = send_sem, recv_sem, phase
        self.copies = []

    def send(self, which, source, target):
        at = (self.phase, len(self.copies))
        copy = pltpu.make_async_remote_copy(
            src_ref=source,
            dst_ref=target,
            send_sem=self.send_sem.at[at],
            recv_sem=self.recv_sem.at[at],
            device_id=self.targets[which],
            device_id_type=MESH,
        )
        copy.start()
        self.copies.append(copy)

    def receive(self):
        for copy in self.copies:
            copy.wait_recv()

    def close(self):
        for copy in self.copies:
            copy.wait_send()


def greet(partners):
    barrier = pltpu.get_barrier_semaphore()
    for partner in partners:
        pl.semaphore_signal(barrier, inc=1, device_id=partner, device_id_type=MESH)


def column_of(grid_ref, first, height, layers):
    return jnp.concatenate([grid_ref[layer, pl.ds(first, height, stride=PITCH), :] for layer in layers], 1)


def put_column(grid_ref, first, layers, values):
    for i, layer in enumerate(layers):
        part = values[:, i * LANE : (i + 1) * LANE]
        grid_ref[layer, pl.ds(first, values.shape[0], stride=PITCH), :] = part


def rows_at(grid_ref, first, height, layers):
    return jnp.concatenate([grid_ref[layer, first : first + height, :] for layer in layers], 1)


def put_rows(grid_ref, first, layers, values):
    for i, layer in enumerate(layers):
        grid_ref[layer, first : first + values.shape[0], :] = values[:, i * LANE : (i + 1) * LANE]


def padded_column(column):
    filler = jnp.zeros((PITCH - column.shape[0], column.shape[1]), f32)
    return jnp.concatenate([column, filler], 0).astype(bf16)


def send_outward(rims, rows_ref, cols_ref, rows_land, cols_land, corner_land, grid_ref, layers, tile):
    for k in range(SHIFT):
        rows_ref[k] = rows_at(grid_ref, (tile + k) * PITCH, PITCH, layers).astype(bf16)
        cols_ref[k] = padded_column(column_of(grid_ref, tile + k, tile + SHIFT, layers))
    rims.send(0, rows_ref, rows_land)
    rims.send(1, cols_ref, cols_land)
    rims.send(2, rows_ref.at[:, pl.ds(PITCH - SUB, SUB)], corner_land)


def receive_outward(rims, rows_land, cols_land, corner_land, grid_ref, layers, tile, target_ref):
    rims.receive()
    corner = tile - (PITCH - SUB)
    for k in range(SHIFT):
        put_rows(grid_ref, k * PITCH, layers, rows_land[k].astype(f32))
    for k in range(SHIFT):
        put_column(grid_ref, k, layers, cols_land[k].astype(f32)[: tile + SHIFT])
    for k in range(SHIFT):
        put_rows(grid_ref, k * PITCH, layers, corner_land[k].astype(f32)[corner : corner + SHIFT])
    for row in range(tile):
        target_ref[row] = rows_at(grid_ref, row * PITCH, tile, layers).astype(bf16)


def window_order(rows, cols):
    spots = [(row, col) for row in range(rows) for col in range(cols)]
    inner = [spot for spot in spots if spot[0] < rows - 1 and spot[1] < cols - 1]
    return inner + [spot for spot in spots if spot not in inner], len(inner)


def place_of(spot, row):
    return (spot[0] * SIDE + row + SHIFT) * PITCH + spot[1] * SIDE + SHIFT


def cut_windows(grid_ref, cell_ref, order, first, last):
    inside = lax.broadcasted_iota(jnp.int32, (CELL, LANE), 0) < SIDE
    for window in range(first, last):
        for layer in range(grid_ref.shape[0]):
            rows = []
            for row in range(SIDE):
                at = place_of(order[window], row)
                rows.append(jnp.where(inside, grid_ref[layer, at : at + CELL, :], 0.0))
            rows.append(jnp.zeros_like(rows[0]))
            lanes = slice(layer * LANE, (layer + 1) * LANE)
            cell_ref[window * SLOTS : (window + 1) * SLOTS, lanes] = jnp.concatenate(rows, 0).astype(bf16)


def join_windows(values, grid_ref, layers, order):
    for window, spot in enumerate(order):
        for row in range(SIDE):
            place = window * SLOTS + row * CELL
            put_rows(grid_ref, place_of(spot, row), layers, values[place : place + SIDE])


def fill_labels(region_ref, wide_ref, label_ref, order):
    rows, cols = region_ref.shape
    wide_ref[:rows, :cols] = region_ref[...].astype(f32)
    area = wide_ref[: -(-rows // CELL) * CELL, :]
    lane = lax.broadcasted_iota(jnp.int32, (1, LANE), 1)
    labels = [jnp.full((1, LANE), -1.0, f32) for _ in order]
    for col in range(cols // SIDE):
        for row in range(SIDE):
            turned = pltpu.roll(area, (row * CELL - col * SIDE) % LANE, 1)
            inside = (lane >= row * CELL) & (lane < row * CELL + SIDE)
            for window, spot in enumerate(order):
                if spot[1] == col:
                    at = spot[0] * SIDE + row
                    labels[window] = jnp.where(inside, turned[at : at + 1, :], labels[window])
    for window in range(len(order)):
        label_ref[window] = labels[window][:, :SLOTS]


def fill_offsets(rel_ref, wide_ref, offset_ref):
    size = rel_ref.shape[0]
    wide_ref[:size, :size] = rel_ref[...].astype(f32)
    lane = lax.broadcasted_iota(jnp.int32, (CELL, LANE), 1)
    row = lax.broadcasted_iota(jnp.int32, (CELL, LANE), 0)
    result = jnp.full((CELL, LANE), -1.0, f32)
    for offset in range(1 - SIDE, SIDE):
        if offset < 0:
            turned = pltpu.roll(wide_ref[-offset * SIDE : CELL - offset * SIDE, :], (SIDE + offset) * CELL, 1)
        else:
            turned = pltpu.roll(wide_ref[:CELL, :], (SIDE + offset) * CELL - offset * SIDE, 1)
        first = (SIDE + offset) * CELL
        result = jnp.where((lane >= first) & (lane < first + SIDE), turned, result)
    offset_ref[...] = jnp.where(row < SIDE, result, -1.0).astype(jnp.int32)


def picks(offset_ref, place):
    labels = lax.broadcasted_iota(jnp.int32, (2 * LANE, LANE), 0)
    return (labels == offset_ref[place : place + 1, :]).astype(f32).astype(bf16)


def fill_bias(offset_ref, table_ref, wide_ref, spread_ref, bias_ref):
    wide_ref[: table_ref.shape[0], : table_ref.shape[1]] = table_ref[...]
    rest = wide_ref[...]
    parts = []
    for _ in range(3):
        part = rest.astype(bf16)
        parts.append(part)
        rest = rest - part.astype(f32)
    parts = jnp.concatenate(parts, 0)
    for place in range(CELL):
        spread = product(parts, picks(offset_ref, place), 1, 0)
        spread = spread[:SUB] + (spread[SUB : 2 * SUB] + spread[2 * SUB :])
        spread_ref[pl.ds(place, HEADS, stride=CELL), :] = spread[:HEADS]
    for head in range(HEADS):
        rows = spread_ref[head * CELL : (head + 1) * CELL, :]
        for row in range(CELL):
            at = head * SLOTS + row * CELL
            if row < SIDE:
                turned = pltpu.roll(rows, LANE - (SIDE - row) * CELL, 1)
                bias_ref[at : at + CELL, :] = turned[:, :SLOTS]
            else:
                bias_ref[at : at + CELL, :] = jnp.zeros((CELL, SLOTS), f32)


def gather_offsets(scores_ref, spread_ref, tiles_ref, first):
    for head in range(HEADS):
        total = jnp.zeros((CELL, LANE), f32)
        for row in range(SIDE):
            at = head * SLOTS + row * CELL
            total = total + pltpu.roll(scores_ref[at : at + CELL, :], (SIDE - row) * CELL, 1)
        spread_ref[head * CELL : (head + 1) * CELL, :] = total
    for place in range(CELL):
        rows = spread_ref[pl.ds(place, HEADS, stride=CELL), :]
        rows = jnp.concatenate([rows, jnp.zeros((SUB - HEADS, LANE), f32)], 0)
        tiles_ref[first + place] = rows.astype(bf16)


def block_kernel(
    windows, streams, slots, limits, order, inner,
    tok_ref, ct_ref, region_in, rel_ref, table_in, wq_ref, wp_ref, w1_ref, w2_ref,
    out_ref, grad_ref, early_out, late_out, table_out, factor_ref,
    region_ref, offset_ref, wide_region, wide_rel, wide_table, cell_ref, grid_ref, out_cells, square_ref, in_cols, in_land, in_cols_land, in_corner_land,
    rows_pack, cols_pack, rows_land, cols_land, corner_land, rim_send, rim_recv,
    bias_ref, spread_ref, scores_ref, normal_ref, qkv_ref, attn_ref, probs_ref, mid_ref, up_ref, gq_ref,
    acc1, acc2, early_in, late_in, early_sum, late_sum, early_land, late_land, send_sem, recv_sem,
):
    exchange = Exchange(
        streams, (early_in, late_in), (early_sum, late_sum), (early_land, late_land), (early_out, late_out),
        send_sem, recv_sem, limits, square_ref,
    )
    rims = [Rims(by, rim_send, rim_recv, phase) for phase, by in enumerate((-1, 1, 1))]
    partners = list(exchange.partners.values()) + list(rims[0].targets) + list(rims[1].targets)
    greet(partners)
    early = [index for index, stream in enumerate(streams) if stream[0] == 0]
    late = [index for index, stream in enumerate(streams) if stream[0] == 1]
    tile, _, channels = tok_ref.shape
    count = cell_ref.shape[0] // SLOTS
    block = windows * SLOTS
    hidden_units = w1_ref.shape[1]
    width = hidden_units // FFN_CHUNKS
    stacked_rows = GROUP * SLOTS
    mask = head_mask()
    mask_low = mask.astype(bf16)
    mine = range(channels // LANE)
    other = range(channels // LANE, 2 * channels // LANE)
    both = range(2 * channels // LANE)
    for row in range(tile):
        put_rows(grid_ref, row * PITCH, mine, tok_ref[row].astype(f32))
        put_rows(grid_ref, row * PITCH, other, ct_ref[row].astype(f32))
    for k in range(SHIFT):
        in_cols[k] = padded_column(column_of(grid_ref, k, tile, both))
    for wide_ref in (wide_region, wide_rel, wide_table):
        wide_ref[...] = jnp.zeros_like(wide_ref)
    fill_labels(region_in, wide_region, region_ref, order)
    fill_offsets(rel_ref, wide_rel, offset_ref)
    fill_bias(offset_ref, table_in, wide_table, spread_ref, bias_ref)
    square_ref[...] = jnp.zeros_like(square_ref)
    pl.semaphore_wait(pltpu.get_barrier_semaphore(), len(partners))
    rims[0].send(0, tok_ref.at[pl.ds(0, SHIFT)], in_land.at[0])
    rims[0].send(0, ct_ref.at[pl.ds(0, SHIFT)], in_land.at[1])
    rims[0].send(1, in_cols, in_cols_land)
    rims[0].send(2, in_cols.at[:, pl.ds(0, SUB)], in_corner_land)
    ready = inner // windows
    cut_windows(grid_ref, cell_ref, order, 0, ready * windows)

    def take_rims():
        rims[0].receive()
        for k in range(SHIFT):
            put_rows(grid_ref, (tile + k) * PITCH, mine, in_land[0, k].astype(f32))
            put_rows(grid_ref, (tile + k) * PITCH, other, in_land[1, k].astype(f32))
            put_column(grid_ref, tile + k, both, in_cols_land[k].astype(f32)[:tile])
            put_column(grid_ref, tile * PITCH + tile + k, both, in_corner_land[k].astype(f32)[:SHIFT])
        cut_windows(grid_ref, cell_ref, order, ready * windows, count)

    acc1[...] = jnp.zeros_like(acc1)
    acc2[...] = jnp.zeros_like(acc2)

    def forward(step, carry):
        pl.when(step == ready)(take_rims)
        rows = pl.ds(pl.multiple_of(step * block, block), block)
        token = cell_ref[rows, :channels].astype(f32)
        upstream = cell_ref[rows, channels:]
        normal, _ = normalize(token)
        normal_low = normal.astype(bf16)
        normal_ref[rows, :] = normal_low
        qkv_ref[rows, :] = product(normal_low, wq_ref[...], 1, 0).astype(bf16)
        for w in range(windows):
            at = pl.ds(pl.multiple_of(step * block + w * SLOTS, SLOTS), SLOTS)
            labels = jnp.broadcast_to(region_ref[step * windows + w], (SLOTS, SLOTS))
            hidden = jnp.where(labels == labels.T, 0.0, -1e30)
            hidden = jnp.concatenate([hidden] * GROUP, 0)
            for g in range(GROUPS):
                lanes = g * LANES
                query = stack_heads(qkv_ref[at, lanes : lanes + LANES], mask_low)
                key = qkv_ref[at, channels + lanes : channels + lanes + LANES]
                value = qkv_ref[at, 2 * channels + lanes : 2 * channels + lanes + LANES]
                bias = bias_ref[g * stacked_rows : (g + 1) * stacked_rows, :]
                scores = product(query, key, 1, 1) * HEAD_DIM ** (-0.5) + bias + hidden
                exponent = jnp.exp(scores - jnp.max(scores, -1, keepdims=True))
                probs = (exponent * (1.0 / jnp.sum(exponent, -1, keepdims=True))).astype(bf16)
                start = ((step * windows + w) * GROUPS + g) * stacked_rows
                probs_ref[pl.ds(pl.multiple_of(start, stacked_rows), stacked_rows), :] = probs
                mixed = product(probs, value, 1, 0)
                attn_ref[at, lanes : lanes + LANES] = gather_heads(mixed, mask).astype(bf16)
        projected = product(attn_ref[rows, :], wp_ref[...], 1, 0).astype(bf16)
        middle = token + projected.astype(f32)
        second, scale = normalize(middle)
        low = second.astype(bf16)
        low_turned = low.T
        up_turned = upstream.T
        total = middle
        back = jnp.zeros_like(middle)
        for c in range(FFN_CHUNKS):
            at = slice(c * width, (c + 1) * width)
            w1 = w1_ref[:, at]
            w2 = w2_ref[at, :]
            pre = product(low, w1, 1, 0)
            cdf = 0.5 * (1.0 + lax.erf(pre * 2.0 ** (-0.5)))
            density = jnp.exp(-0.5 * pre * pre) * (2.0 * math.pi) ** (-0.5)
            active = (pre * cdf).astype(bf16)
            total = total + product(active, w2, 1, 0)
            acc2[:, at] += product(up_turned, active, 1, 0)
            grad_pre = (product(upstream, w2, 1, 1) * (cdf + pre * density)).astype(bf16)
            acc1[:, at] += product(low_turned, grad_pre, 1, 0)
            back = back + product(grad_pre, w1, 1, 1)
        out_cells[rows, :] = total
        mid_ref[rows, :] = upstream.astype(f32) + normalize_back(second, scale, back)
        return carry

    lax.fori_loop(0, count // windows, forward, 0)

    mid_low = mid_ref[...].astype(bf16)
    to_tiles(acc1[...], early_in, 0)
    to_tiles(acc2[...].T, early_in, acc1.size // TILE)
    used = 2 * acc1.size // TILE
    to_tiles(product(attn_ref[...], mid_low, 0, 0), early_in, used)
    used += channels * channels // TILE
    if used < early_in.shape[0]:
        early_in[used:] = jnp.zeros((early_in.shape[0] - used, SUB, LANE), bf16)
    for index in early:
        exchange.start(index)
    join_windows(out_cells, grid_ref, mine, order)
    landings = [(rows_land.at[i], cols_land.at[i], corner_land.at[i]) for i in range(2)]
    send_outward(rims[1], rows_pack.at[0], cols_pack.at[0], *landings[0], grid_ref, mine, tile)
    up_ref[...] = product(mid_low, wp_ref[...], 1, 1).astype(bf16)
    scores_ref[...] = jnp.zeros_like(scores_ref)

    def backward(step, carry):
        for slot, moves in enumerate(slots):
            if moves:
                @pl.when(step == slot)
                def _(moves=moves):
                    for index in moves:
                        exchange.advance(index)

        for w in range(PAIR):
            at = pl.ds(pl.multiple_of((step * PAIR + w) * SLOTS, SLOTS), SLOTS)
            for g in range(GROUPS):
                first = slice(g * LANES, (g + 1) * LANES)
                second = slice(channels + g * LANES, channels + (g + 1) * LANES)
                third = slice(2 * channels + g * LANES, 2 * channels + (g + 1) * LANES)
                rows = slice(g * stacked_rows, (g + 1) * stacked_rows)
                query = stack_heads(qkv_ref[at, first], mask_low)
                key = qkv_ref[at, second]
                value = qkv_ref[at, third]
                upstream = stack_heads(up_ref[at, first], mask_low)
                start = ((step * PAIR + w) * GROUPS + g) * stacked_rows
                low = probs_ref[pl.ds(pl.multiple_of(start, stacked_rows), stacked_rows), :]
                probs = low.astype(f32)
                grad_probs = product(upstream, value, 1, 1)
                inner = jnp.sum(probs * grad_probs, -1, keepdims=True)
                grad_scores = probs * (grad_probs - inner)
                scores_ref[rows, :SLOTS] += grad_scores
                scaled = (grad_scores * HEAD_DIM ** (-0.5)).astype(bf16)
                gq_ref[at, first] = gather_heads(product(scaled, key, 1, 0), mask).astype(bf16)
                gq_ref[at, second] = product(scaled, query, 0, 0).astype(bf16)
                gq_ref[at, third] = product(low, upstream, 0, 0).astype(bf16)
        return carry

    lax.fori_loop(0, count // PAIR, backward, 0)

    normal_turned = normal_ref[...].T
    to_tiles(product(normal_turned, gq_ref[...], 1, 0), late_in, 0)
    used = 3 * channels * channels // TILE
    gather_offsets(scores_ref, spread_ref, late_in, used)
    used += CELL
    if used < late_in.shape[0]:
        late_in[used:] = jnp.zeros((late_in.shape[0] - used, SUB, LANE), bf16)
    for index in late:
        exchange.start(index)

    def finish_tokens(step, carry):
        rows = pl.ds(pl.multiple_of(step * block, block), block)
        normal, scale = normalize(cell_ref[rows, :channels].astype(f32))
        grad_normed = product(gq_ref[rows, :], wq_ref[...], 1, 1).astype(bf16).astype(f32)
        out_cells[rows, :] = mid_ref[rows, :] + normalize_back(normal, scale, grad_normed)
        return carry

    lax.fori_loop(0, count // windows, finish_tokens, 0)
    join_windows(out_cells, grid_ref, other, order)
    send_outward(rims[2], rows_pack.at[1], cols_pack.at[1], *landings[1], grid_ref, other, tile)
    receive_outward(rims[1], *landings[0], grid_ref, mine, tile, out_ref)
    for index in late + early:
        exchange.advance(index)
    receive_outward(rims[2], *landings[1], grid_ref, other, tile, grad_ref)
    exchange.drain(late + early)
    table = jnp.zeros((SUB, 2 * LANE), f32)
    for place in range(CELL):
        table = table + product(late_out[limits[1] + place], picks(offset_ref, place), 1, 1)
    table_out[...] = table
    norm_sq = jnp.sum(square_ref[...]) + jnp.sum(table * table)
    norm_sq = jnp.full((SUB // 2, LANE), norm_sq, f32)
    factor_ref[...] = jnp.minimum(1.0, math.sqrt(PARAMS) / (jnp.sqrt(norm_sq) + 1e-06))
    exchange.close()
    for rim in rims:
        rim.close()


def finish_kernel(
    pieces, block_in, grad_in, early_ref, late_ref, table_ref, factor_ref,
    block_out, token_out, gq_ref, gp_ref, g1_ref, g2_ref, table_out,
    block_full, token_full, tiles, gq_full, gp_full, g1_full, g2_full, in_sem, out_sem,
):
    sources = (early_ref, late_ref)
    results = ((gq_ref, gq_full), (gp_ref, gp_full), (g1_ref, g1_full), (g2_ref, g2_full))
    loads = []
    at = 0
    for i, (group, first, length, _, _, _) in enumerate(pieces):
        load = pltpu.make_async_copy(
            sources[group].at[pl.ds(first, length)], tiles.at[pl.ds(at, length)], in_sem.at[i]
        )
        load.start()
        loads.append((load, at))
        at += length
    passed = ((block_in, block_full, block_out), (grad_in, token_full, token_out))
    for i, (source, full, _) in enumerate(passed):
        load = pltpu.make_async_copy(source, full, in_sem.at[len(pieces) + i])
        load.start()
        loads.append((load, 0))
    factor = factor_ref[:1]
    stores = []
    for i, (group, first, length, which, column, columns) in enumerate(pieces):
        load, at = loads[i]
        load.wait()
        target, full = results[which]
        rows = full.shape[0]
        high = rows // SUB
        for k in range(columns):
            block = tiles[at + k * high : at + (k + 1) * high].reshape(rows, LANE).astype(f32)
            full[:, (column + k) * LANE : (column + k + 1) * LANE] = block * factor
        lanes = pl.ds(column * LANE, columns * LANE)
        store = pltpu.make_async_copy(full.at[:, lanes], target.at[:, lanes], out_sem.at[i])
        store.start()
        stores.append(store)
    for i, (_, full, target) in enumerate(passed):
        loads[len(pieces) + i][0].wait()
        store = pltpu.make_async_copy(full, target, out_sem.at[len(pieces) + i])
        store.start()
        stores.append(store)
    table = table_ref[...] * jnp.concatenate([factor] * 2, 1)
    table_out[...] = table[: table_out.shape[0], : table_out.shape[1]]
    for store in stores:
        store.wait()


def pieces_of(channels, ffn):
    pieces = []
    starts = [0, 0]
    for group, which, rows, lanes, step in (
        (0, 2, channels, ffn, 3), (0, 3, ffn, channels, 1), (0, 1, channels, channels, 3), (1, 0, channels, 3 * channels, 3),
    ):
        for column in range(0, lanes // LANE, step):
            length = rows // SUB * step
            pieces.append((group, starts[group], length, which, column, step))
            starts[group] += length
    return pieces


def local(tokens, cotangent, w_qkv, w_proj, w_fc1, w_fc2, bias_table, rel_index, region):
    tile_rows, tile_cols, channels = tokens.shape
    ffn = w_fc1.shape[1]
    count = (tile_rows // SIDE) * (tile_cols // SIDE)
    windows = math.gcd(count, 4)
    total = count * SLOTS

    order, inner = window_order(tile_rows // SIDE, tile_cols // SIDE)
    across = (lax.axis_size("ha"), lax.axis_size("wa"))
    devices = across[0] * across[1]
    early_tiles = padded_tiles((2 * channels * ffn + channels * channels) // TILE, devices)
    late_tiles = padded_tiles(3 * channels * channels // TILE + CELL, devices)
    orders = link_orders(*across)
    streams = split_streams(0, early_tiles, devices, STREAMS[0], orders)
    early_count = len(streams)
    streams += split_streams(1, late_tiles, devices, STREAMS[1], orders)
    slots = [[index for index in moves if index < early_count] for moves in SLOT_MOVES[: count // PAIR]]

    shape = jax.ShapeDtypeStruct
    early = (early_tiles, SUB, LANE)
    late = (late_tiles, SUB, LANE)
    in_vmem = pl.BlockSpec(memory_space=pltpu.VMEM)
    semaphores = pltpu.SemaphoreType.DMA((len(streams), 2 * len(orders[0])))
    vmem_limit = 63 * 1024 * 1024
    limits = (early_tiles, 3 * channels * channels // TILE)
    vmem = pltpu.VMEM
    summed = pl.pallas_call(
        functools.partial(block_kernel, windows, streams, slots, limits, order, inner),
        name="block",
        out_shape=[
            shape(tokens.shape, bf16), shape(tokens.shape, bf16), shape(early, bf16), shape(late, bf16),
            shape((SUB, 2 * LANE), f32), shape((SUB // 2, LANE), f32),
        ],
        in_specs=[in_vmem] * 9,
        out_specs=[in_vmem] * 6,
        scratch_shapes=[
            vmem((count, 1, SLOTS), f32),
            vmem((CELL, LANE), jnp.int32),
            vmem((LANE, LANE), f32),
            vmem((LANE, LANE), f32),
            vmem((SUB, 2 * LANE), f32),
            vmem((total, 2 * channels), bf16),
            vmem((2 * channels // LANE, (tile_rows + SHIFT) * PITCH, LANE), f32),
            vmem((total, channels), f32),
            vmem((SUB, LANE), f32),
            vmem((SHIFT, PITCH, 2 * channels), bf16),
            vmem((2, SHIFT, tile_cols, channels), bf16),
            vmem((SHIFT, PITCH, 2 * channels), bf16),
            vmem((SHIFT, SUB, 2 * channels), bf16),
            vmem((2, SHIFT, PITCH, channels), bf16),
            vmem((2, SHIFT, PITCH, channels), bf16),
            vmem((2, SHIFT, PITCH, channels), bf16),
            vmem((2, SHIFT, PITCH, channels), bf16),
            vmem((2, SHIFT, SUB, channels), bf16),
            pltpu.SemaphoreType.DMA((3, 4)),
            pltpu.SemaphoreType.DMA((3, 4)),
            vmem((HEADS * SLOTS, SLOTS), f32),
            vmem((HEADS * CELL, LANE), f32),
            vmem((HEADS * SLOTS, LANE), f32),
            vmem((total, channels), bf16),
            vmem((total, 3 * channels), bf16),
            vmem((total, channels), bf16),
            vmem((count * HEADS * SLOTS, SLOTS), bf16),
            vmem((total, channels), f32),
            vmem((total, channels), bf16),
            vmem((total, 3 * channels), bf16),
            vmem((channels, ffn), f32),
            vmem((channels, ffn), f32),
        ] + [vmem(group, bf16) for group in (early, late)] * 3 + [semaphores] * 2,
        compiler_params=pltpu.CompilerParams(
            collective_id=0, has_side_effects=True, vmem_limit_bytes=vmem_limit
        ),
        cost_estimate=pl.CostEstimate(
            flops=36_000_000_000, bytes_accessed=20_000_000, transcendentals=5_000_000
        ),
    )(tokens, cotangent, region, rel_index, bias_table.T, w_qkv, w_proj, w_fc1, w_fc2)

    pieces = pieces_of(channels, ffn)
    in_place = pl.BlockSpec(memory_space=pl.ANY)
    results = [(channels, 3 * channels), (channels, channels), (channels, ffn), (ffn, channels)]
    block_out, token_grad, gq, gp, g1, g2, table = pl.pallas_call(
        functools.partial(finish_kernel, pieces),
        name="finish",
        out_shape=[shape(tokens.shape, bf16)] * 2
        + [shape(result, f32) for result in results]
        + [shape(bias_table.T.shape, f32)],
        in_specs=[in_place] * 4 + [in_vmem] * 2,
        out_specs=[in_place] * 6 + [in_vmem],
        scratch_shapes=[vmem(tokens.shape, bf16)] * 2
        + [vmem((sum(piece[2] for piece in pieces), SUB, LANE), bf16)]
        + [vmem(result, f32) for result in results]
        + [pltpu.SemaphoreType.DMA((len(pieces) + 2,))] * 2,
        compiler_params=pltpu.CompilerParams(vmem_limit_bytes=vmem_limit),
    )(*summed)
    return (block_out, token_grad, gq, gp, g1, g2, table.T)


def solution(mesh):
    placed = (P("ha", "wa", None), P("ha", "wa", None), P(), P(), P(), P(), P(), P(), P("ha", "wa"))
    return jax.shard_map(
        local,
        mesh=mesh,
        in_specs=placed,
        out_specs=(P("ha", "wa", None), P("ha", "wa", None), P(), P(), P(), P(), P()),
        check_vma=False,
    )
```

```python
import functools
import math

import jax
import jax.numpy as jnp
from jax import lax
from jax.experimental import pallas as pl
from jax.experimental.pallas import tpu as pltpu
from jax.sharding import PartitionSpec as P

HEADS = 12
SIDE = 7
SHIFT = 3
HEAD_DIM = 32
TABLE = 169
PARAMS = 1771500
CELL = 8
SLOTS = CELL * CELL
GROUP = 4
LANES = GROUP * HEAD_DIM
GROUPS = HEADS // GROUP
FFN_CHUNKS = 3
SUB = 16
LANE = 128
TILE = SUB * LANE
EARLY_PLAN = (('a', 4), ('b', 4), ('c', 5), ('a', 4), ('b', 4))
LATE_PLAN = (('d', 1), ('e', 1))
PAIR = 2
TOKEN_MOVES = ('e', 'l', '', 'e')
ROUNDS_BY_SLOT = (0, 1, 1, 1.4, 2, 2.4, 3, 3.4)
MESH = pl.DeviceIdType.MESH
PITCH = 32

epsilon = 1e-05
highest = lax.Precision.HIGHEST
f32 = jnp.float32
bf16 = jnp.bfloat16


def normalize(values):
    average = jnp.mean(values, -1, keepdims=True)
    centred = values - average
    inverse = lax.rsqrt(jnp.mean(centred * centred, -1, keepdims=True) + epsilon)
    return (centred * inverse, inverse)


def normalize_back(normal_rows, inverse, upstream):
    up_mean = jnp.mean(upstream, -1, keepdims=True)
    cross_mean = jnp.mean(upstream * normal_rows, -1, keepdims=True)
    return inverse * (upstream - up_mean - normal_rows * cross_mean)


def product(left, right, left_dim, right_dim):
    return lax.dot_general(
        left, right, (((left_dim,), (right_dim,)), ((), ())), preferred_element_type=f32
    )


def head_mask():
    shape = (GROUP * SLOTS, LANES)
    row_head = lax.broadcasted_iota(jnp.int32, shape, 0) // SLOTS
    lane_head = lax.broadcasted_iota(jnp.int32, shape, 1) // HEAD_DIM
    return (row_head == lane_head).astype(f32)


def stack_heads(rows, mask):
    return jnp.concatenate([rows] * GROUP, 0) * mask


def gather_heads(stacked, mask):
    kept = stacked * mask
    total = kept[:SLOTS]
    for head in range(1, GROUP):
        total = total + kept[head * SLOTS : (head + 1) * SLOTS]
    return total


def to_tiles(values, tiles_ref, at):
    rows, lanes = values.shape
    high = rows // SUB
    low = values.astype(bf16)
    for column in range(lanes // LANE):
        block = low[:, column * LANE : (column + 1) * LANE].reshape(high, SUB, LANE)
        tiles_ref[at + column * high : at + (column + 1) * high] = block


def digits_of(axis, size, stride, most):
    digits = []
    while stride < size:
        radix = min(most, size // stride)
        digits.append((axis, stride, radix))
        stride *= radix
    return digits


def link_orders(across_ha, across_wa):
    core = digits_of("wa", 2, 1, 2)
    near = digits_of("ha", across_ha, 1, 2)
    near_wide = digits_of("ha", across_ha, 1, 4)
    far = digits_of("wa", across_wa, 2, 4)
    far_slim = digits_of("wa", across_wa, 2, 2)
    orders = {
        "a": core + near + far,
        "b": core + near[::-1] + far,
        "c": core + far + near,
        "d": core + near_wide + far,
        "e": core + far + near_wide,
        "s": core + near + far_slim,
        "t": core + near[::-1] + far_slim,
        "u": core + far_slim + near,
    }
    return orders


def split_streams(group, tiles, devices, plan, orders):
    units = tiles // devices
    total = sum(weight for _, weight in plan)
    streams = []
    base = 0
    passed = 0
    for name, weight in plan:
        passed += weight
        size = (units * passed + total // 2) // total * devices - base
        if size:
            streams.append((group, base, size, orders[name]))
        base += size
    return streams


def slot_moves(streams, slots):
    moves = []
    done = 0
    for slot in range(slots):
        until = int(ROUNDS_BY_SLOT[min(slot, len(ROUNDS_BY_SLOT) - 1)] * streams)
        moves.append([index % streams for index in range(done, until)])
        done = max(done, until)
    return moves


def padded_tiles(tiles, devices):
    return -(-tiles // devices) * devices


def chunk_of(count):
    return max(size for size in range(1, 17) if count % size == 0)


class Exchange:
    def __init__(self, streams, sources, sums, landing, totals, send_sem, recv_sem, limits, square_ref):
        self.streams = streams
        self.sources, self.sums, self.landing, self.totals = sources, sums, landing, totals
        self.send_sem, self.recv_sem = send_sem, recv_sem
        self.limits, self.square_ref = limits, square_ref
        self.done = [0] * len(streams)
        self.places = []
        self.partners = {}
        for group, base, size, order in streams:
            places = []
            low = base
            arrive = base
            for axis, stride, radix in order:
                size = size // radix
                me = lax.axis_index(axis)
                digit = (me // stride) % radix
                sends = []
                for k in range(1, radix):
                    ahead = (digit + k) % radix
                    behind = (digit + radix - k) % radix
                    partner = {axis: me + (ahead - digit) * stride}
                    self.partners[axis, stride, radix, k] = partner
                    sends.append((partner, low + ahead * size, low + behind * size, arrive))
                    arrive += size
                low = low + digit * size
                places.append((low, size, sends))
            self.places.append(places)

    def rounds(self, index):
        return len(self.places[index])

    def copies(self, index, slot):
        group = self.streams[index][0]
        rounds = self.rounds(index)
        keep, size, sends = self.places[index][slot if slot < rounds else 2 * rounds - 1 - slot]
        result = []
        for k, (partner, give, _, arrive) in enumerate(sends):
            if slot < rounds:
                source = (self.sums if slot else self.sources)[group].at[pl.ds(give, size)]
                target = self.landing[group].at[pl.ds(arrive, size)]
            else:
                source = self.totals[group].at[pl.ds(keep, size)]
                target = source
            result.append(
                pltpu.make_async_remote_copy(
                    src_ref=source,
                    dst_ref=target,
                    send_sem=self.send_sem.at[index, slot, k],
                    recv_sem=self.recv_sem.at[index, slot, k],
                    device_id=partner,
                    device_id_type=MESH,
                )
            )
        return result

    def add(self, index, step):
        group = self.streams[index][0]
        keep, size, sends = self.places[index][step]
        source = (self.sums if step else self.sources)[group]
        target = (self.sums if step < self.rounds(index) - 1 else self.totals)[group]
        landing = self.landing[group]
        chunk = chunk_of(size)

        def body(i, carry):
            at = pl.ds(keep + i * chunk, chunk)
            total = source[at].astype(f32)
            for _, _, _, arrive in sends:
                total = total + landing[pl.ds(arrive + i * chunk, chunk)].astype(f32)
            target[at] = total.astype(bf16)
            return carry

        lax.fori_loop(0, size // chunk, body, 0)

    def start(self, index, slot=0):
        for copy in self.copies(index, slot):
            copy.start()

    def advance(self, index):
        slot = self.done[index]
        rounds = self.rounds(index)
        if slot == 2 * rounds:
            return
        for copy in self.copies(index, slot):
            copy.wait_recv()
        if slot < rounds:
            self.add(index, slot)
        if slot + 1 < 2 * rounds:
            self.start(index, slot + 1)
        keep, size, sends = self.places[index][slot if slot < rounds else 2 * rounds - 1 - slot]
        if slot == rounds - 1:
            self.square(index, keep, size)
        elif slot >= rounds:
            for _, _, behind, _ in sends:
                self.square(index, behind, size)
        self.done[index] = slot + 1

    def square(self, index, first, length):
        group = self.streams[index][0]
        totals = self.totals[group]
        chunk = chunk_of(length)

        def body(i, total):
            at = first + i * chunk
            block = totals[pl.ds(at, chunk)].astype(f32)
            inside = lax.broadcasted_iota(jnp.int32, block.shape, 0) + at < self.limits[group]
            return total + jnp.sum(jnp.where(inside, block * block, 0.0), 0)

        total = lax.fori_loop(0, length // chunk, body, jnp.zeros((SUB, LANE), f32))
        self.square_ref[...] += total

    def drain(self, order):
        while any(self.done[index] < 2 * self.rounds(index) for index in order):
            for index in order:
                self.advance(index)

    def close(self):
        for index in range(len(self.streams)):
            for slot in range(2 * self.rounds(index)):
                for copy in self.copies(index, slot):
                    copy.wait_send()


class Rims:
    def __init__(self, by, send_sem, recv_sem, phase):
        spots = {}
        for axis in ("ha", "wa"):
            count = lax.axis_size(axis)
            spots[axis] = (lax.axis_index(axis) + by + count) % count
        self.targets = ({"ha": spots["ha"]}, {"wa": spots["wa"]}, spots)
        self.send_sem, self.recv_sem, self.phase = send_sem, recv_sem, phase
        self.copies = []

    def send(self, which, source, target):
        at = (self.phase, len(self.copies))
        copy = pltpu.make_async_remote_copy(
            src_ref=source,
            dst_ref=target,
            send_sem=self.send_sem.at[at],
            recv_sem=self.recv_sem.at[at],
            device_id=self.targets[which],
            device_id_type=MESH,
        )
        copy.start()
        self.copies.append(copy)

    def receive(self):
        for copy in self.copies:
            copy.wait_recv()

    def close(self):
        for copy in self.copies:
            copy.wait_send()


def greet(partners):
    barrier = pltpu.get_barrier_semaphore()
    for partner in partners:
        pl.semaphore_signal(barrier, inc=1, device_id=partner, device_id_type=MESH)


def column_of(grid_ref, first, height, layers):
    return jnp.concatenate([grid_ref[layer, pl.ds(first, height, stride=PITCH), :] for layer in layers], 1)


def put_column(grid_ref, first, layers, values):
    for i, layer in enumerate(layers):
        part = values[:, i * LANE : (i + 1) * LANE]
        grid_ref[layer, pl.ds(first, values.shape[0], stride=PITCH), :] = part


def rows_at(grid_ref, first, height, layers):
    return jnp.concatenate([grid_ref[layer, first : first + height, :] for layer in layers], 1)


def put_rows(grid_ref, first, layers, values):
    for i, layer in enumerate(layers):
        grid_ref[layer, first : first + values.shape[0], :] = values[:, i * LANE : (i + 1) * LANE]


def padded_column(column):
    filler = jnp.zeros((PITCH - column.shape[0], column.shape[1]), f32)
    return jnp.concatenate([column, filler], 0).astype(bf16)


def send_outward(rims, rows_ref, cols_ref, rows_land, cols_land, corner_land, grid_ref, layers, tile):
    for k in range(SHIFT):
        rows_ref[k] = rows_at(grid_ref, (tile + k) * PITCH, PITCH, layers).astype(bf16)
        cols_ref[k] = padded_column(column_of(grid_ref, tile + k, tile + SHIFT, layers))
    rims.send(0, rows_ref, rows_land)
    rims.send(1, cols_ref, cols_land)
    rims.send(2, rows_ref.at[:, pl.ds(PITCH - SUB, SUB)], corner_land)


def receive_outward(rims, rows_land, cols_land, corner_land, grid_ref, layers, tile, target_ref):
    rims.receive()
    corner = tile - (PITCH - SUB)
    for k in range(SHIFT):
        put_rows(grid_ref, k * PITCH, layers, rows_land[k].astype(f32))
    for k in range(SHIFT):
        put_column(grid_ref, k, layers, cols_land[k].astype(f32)[: tile + SHIFT])
    for k in range(SHIFT):
        put_rows(grid_ref, k * PITCH, layers, corner_land[k].astype(f32)[corner : corner + SHIFT])
    for row in range(tile):
        target_ref[row] = rows_at(grid_ref, row * PITCH, tile, layers).astype(bf16)


def window_order(rows, cols):
    spots = [(row, col) for row in range(rows) for col in range(cols)]
    inner = [spot for spot in spots if spot[0] < rows - 1 and spot[1] < cols - 1]
    return inner + [spot for spot in spots if spot not in inner], len(inner)


def place_of(spot, row):
    return (spot[0] * SIDE + row + SHIFT) * PITCH + spot[1] * SIDE + SHIFT


def cut_windows(grid_ref, cell_ref, order, first, last):
    inside = lax.broadcasted_iota(jnp.int32, (CELL, LANE), 0) < SIDE
    for window in range(first, last):
        for layer in range(grid_ref.shape[0]):
            rows = []
            for row in range(SIDE):
                at = place_of(order[window], row)
                rows.append(jnp.where(inside, grid_ref[layer, at : at + CELL, :], 0.0))
            rows.append(jnp.zeros_like(rows[0]))
            lanes = slice(layer * LANE, (layer + 1) * LANE)
            cell_ref[window * SLOTS : (window + 1) * SLOTS, lanes] = jnp.concatenate(rows, 0).astype(bf16)


def join_windows(values, grid_ref, layers, order):
    for window, spot in enumerate(order):
        for row in range(SIDE):
            place = window * SLOTS + row * CELL
            put_rows(grid_ref, place_of(spot, row), layers, values[place : place + SIDE])


def fill_labels(region_ref, wide_ref, label_ref, order):
    rows, cols = region_ref.shape
    wide_ref[:rows, :cols] = region_ref[...].astype(f32)
    area = wide_ref[: -(-rows // CELL) * CELL, :]
    lane = lax.broadcasted_iota(jnp.int32, (1, LANE), 1)
    labels = [jnp.full((1, LANE), -1.0, f32) for _ in order]
    for col in range(cols // SIDE):
        for row in range(SIDE):
            turned = pltpu.roll(area, (row * CELL - col * SIDE) % LANE, 1)
            inside = (lane >= row * CELL) & (lane < row * CELL + SIDE)
            for window, spot in enumerate(order):
                if spot[1] == col:
                    at = spot[0] * SIDE + row
                    labels[window] = jnp.where(inside, turned[at : at + 1, :], labels[window])
    for window in range(len(order)):
        label_ref[window] = labels[window][:, :SLOTS]


def fill_offsets(rel_ref, wide_ref, offset_ref):
    size = rel_ref.shape[0]
    wide_ref[:size, :size] = rel_ref[...].astype(f32)
    lane = lax.broadcasted_iota(jnp.int32, (CELL, LANE), 1)
    row = lax.broadcasted_iota(jnp.int32, (CELL, LANE), 0)
    result = jnp.full((CELL, LANE), -1.0, f32)
    for offset in range(1 - SIDE, SIDE):
        if offset < 0:
            turned = pltpu.roll(wide_ref[-offset * SIDE : CELL - offset * SIDE, :], (SIDE + offset) * CELL, 1)
        else:
            turned = pltpu.roll(wide_ref[:CELL, :], (SIDE + offset) * CELL - offset * SIDE, 1)
        first = (SIDE + offset) * CELL
        result = jnp.where((lane >= first) & (lane < first + SIDE), turned, result)
    offset_ref[...] = jnp.where(row < SIDE, result, -1.0).astype(jnp.int32)


def picks(offset_ref, place):
    labels = lax.broadcasted_iota(jnp.int32, (2 * LANE, LANE), 0)
    return (labels == offset_ref[place : place + 1, :]).astype(f32).astype(bf16)


def fill_bias(offset_ref, table_ref, wide_ref, spread_ref, bias_ref):
    wide_ref[: table_ref.shape[0], : table_ref.shape[1]] = table_ref[...]
    rest = wide_ref[...]
    parts = []
    for _ in range(3):
        part = rest.astype(bf16)
        parts.append(part)
        rest = rest - part.astype(f32)
    parts = jnp.concatenate(parts, 0)
    for place in range(CELL):
        spread = product(parts, picks(offset_ref, place), 1, 0)
        spread = spread[:SUB] + (spread[SUB : 2 * SUB] + spread[2 * SUB :])
        spread_ref[pl.ds(place, HEADS, stride=CELL), :] = spread[:HEADS]
    for head in range(HEADS):
        rows = spread_ref[head * CELL : (head + 1) * CELL, :]
        for row in range(CELL):
            at = head * SLOTS + row * CELL
            if row < SIDE:
                turned = pltpu.roll(rows, LANE - (SIDE - row) * CELL, 1)
                bias_ref[at : at + CELL, :] = turned[:, :SLOTS]
            else:
                bias_ref[at : at + CELL, :] = jnp.zeros((CELL, SLOTS), f32)


def gather_offsets(scores_ref, spread_ref, tiles_ref, first):
    for head in range(HEADS):
        total = jnp.zeros((CELL, LANE), f32)
        for row in range(SIDE):
            at = head * SLOTS + row * CELL
            total = total + pltpu.roll(scores_ref[at : at + CELL, :], (SIDE - row) * CELL, 1)
        spread_ref[head * CELL : (head + 1) * CELL, :] = total
    for place in range(CELL):
        rows = spread_ref[pl.ds(place, HEADS, stride=CELL), :]
        rows = jnp.concatenate([rows, jnp.zeros((SUB - HEADS, LANE), f32)], 0)
        tiles_ref[first + place] = rows.astype(bf16)


def block_kernel(
    windows, streams, slots, limits, order, inner,
    tok_ref, ct_ref, region_in, rel_ref, table_in, wq_ref, wp_ref, w1_ref, w2_ref,
    out_ref, grad_ref, early_out, late_out, table_out, factor_ref,
    region_ref, offset_ref, wide_region, wide_rel, wide_table, cell_ref, grid_ref, out_cells, square_ref, in_cols, in_land, in_cols_land, in_corner_land,
    rows_pack, cols_pack, rows_land, cols_land, corner_land, rim_send, rim_recv,
    bias_ref, spread_ref, scores_ref, normal_ref, qkv_ref, attn_ref, probs_ref, mid_ref, up_ref, gq_ref,
    acc1, acc2, early_in, late_in, early_sum, late_sum, early_land, late_land, send_sem, recv_sem,
):
    exchange = Exchange(
        streams, (early_in, late_in), (early_sum, late_sum), (early_land, late_land), (early_out, late_out),
        send_sem, recv_sem, limits, square_ref,
    )
    rims = [Rims(by, rim_send, rim_recv, phase) for phase, by in enumerate((-1, 1, 1))]
    partners = list(exchange.partners.values()) + list(rims[0].targets) + list(rims[1].targets)
    greet(partners)
    early = [index for index, stream in enumerate(streams) if stream[0] == 0]
    late = [index for index, stream in enumerate(streams) if stream[0] == 1]
    tile, _, channels = tok_ref.shape
    count = cell_ref.shape[0] // SLOTS
    block = windows * SLOTS
    hidden_units = w1_ref.shape[1]
    width = hidden_units // FFN_CHUNKS
    stacked_rows = GROUP * SLOTS
    mask = head_mask()
    mask_low = mask.astype(bf16)
    mine = range(channels // LANE)
    other = range(channels // LANE, 2 * channels // LANE)
    both = range(2 * channels // LANE)
    for row in range(tile):
        put_rows(grid_ref, row * PITCH, mine, tok_ref[row].astype(f32))
        put_rows(grid_ref, row * PITCH, other, ct_ref[row].astype(f32))
    for k in range(SHIFT):
        in_cols[k] = padded_column(column_of(grid_ref, k, tile, both))
    for wide_ref in (wide_region, wide_rel, wide_table):
        wide_ref[...] = jnp.zeros_like(wide_ref)
    fill_labels(region_in, wide_region, region_ref, order)
    fill_offsets(rel_ref, wide_rel, offset_ref)
    fill_bias(offset_ref, table_in, wide_table, spread_ref, bias_ref)
    square_ref[...] = jnp.zeros_like(square_ref)
    pl.semaphore_wait(pltpu.get_barrier_semaphore(), len(partners))
    rims[0].send(0, tok_ref.at[pl.ds(0, SHIFT)], in_land.at[0])
    rims[0].send(0, ct_ref.at[pl.ds(0, SHIFT)], in_land.at[1])
    rims[0].send(1, in_cols, in_cols_land)
    rims[0].send(2, in_cols.at[:, pl.ds(0, SUB)], in_corner_land)
    ready = inner // windows
    cut_windows(grid_ref, cell_ref, order, 0, ready * windows)

    def take_rims():
        rims[0].receive()
        for k in range(SHIFT):
            put_rows(grid_ref, (tile + k) * PITCH, mine, in_land[0, k].astype(f32))
            put_rows(grid_ref, (tile + k) * PITCH, other, in_land[1, k].astype(f32))
            put_column(grid_ref, tile + k, both, in_cols_land[k].astype(f32)[:tile])
            put_column(grid_ref, tile * PITCH + tile + k, both, in_corner_land[k].astype(f32)[:SHIFT])
        cut_windows(grid_ref, cell_ref, order, ready * windows, count)

    acc1[...] = jnp.zeros_like(acc1)
    acc2[...] = jnp.zeros_like(acc2)

    def forward(step, carry):
        pl.when(step == ready)(take_rims)
        rows = pl.ds(pl.multiple_of(step * block, block), block)
        token = cell_ref[rows, :channels].astype(f32)
        upstream = cell_ref[rows, channels:]
        normal, _ = normalize(token)
        normal_low = normal.astype(bf16)
        normal_ref[rows, :] = normal_low
        qkv_ref[rows, :] = product(normal_low, wq_ref[...], 1, 0).astype(bf16)
        for w in range(windows):
            at = pl.ds(pl.multiple_of(step * block + w * SLOTS, SLOTS), SLOTS)
            labels = jnp.broadcast_to(region_ref[step * windows + w], (SLOTS, SLOTS))
            hidden = jnp.where(labels == labels.T, 0.0, -1e30)
            hidden = jnp.concatenate([hidden] * GROUP, 0)
            for g in range(GROUPS):
                lanes = g * LANES
                query = stack_heads(qkv_ref[at, lanes : lanes + LANES], mask_low)
                key = qkv_ref[at, channels + lanes : channels + lanes + LANES]
                value = qkv_ref[at, 2 * channels + lanes : 2 * channels + lanes + LANES]
                bias = bias_ref[g * stacked_rows : (g + 1) * stacked_rows, :]
                scores = product(query, key, 1, 1) * HEAD_DIM ** (-0.5) + bias + hidden
                exponent = jnp.exp(scores - jnp.max(scores, -1, keepdims=True))
                probs = (exponent * (1.0 / jnp.sum(exponent, -1, keepdims=True))).astype(bf16)
                start = ((step * windows + w) * GROUPS + g) * stacked_rows
                probs_ref[pl.ds(pl.multiple_of(start, stacked_rows), stacked_rows), :] = probs
                mixed = product(probs, value, 1, 0)
                attn_ref[at, lanes : lanes + LANES] = gather_heads(mixed, mask).astype(bf16)
        projected = product(attn_ref[rows, :], wp_ref[...], 1, 0).astype(bf16)
        middle = token + projected.astype(f32)
        second, scale = normalize(middle)
        low = second.astype(bf16)
        low_turned = low.T
        up_turned = upstream.T
        total = middle
        back = jnp.zeros_like(middle)
        for c in range(FFN_CHUNKS):
            at = slice(c * width, (c + 1) * width)
            w1 = w1_ref[:, at]
            w2 = w2_ref[at, :]
            pre = product(low, w1, 1, 0)
            cdf = 0.5 * (1.0 + lax.erf(pre * 2.0 ** (-0.5)))
            density = jnp.exp(-0.5 * pre * pre) * (2.0 * math.pi) ** (-0.5)
            active = (pre * cdf).astype(bf16)
            total = total + product(active, w2, 1, 0)
            acc2[:, at] += product(up_turned, active, 1, 0)
            grad_pre = (product(upstream, w2, 1, 1) * (cdf + pre * density)).astype(bf16)
            acc1[:, at] += product(low_turned, grad_pre, 1, 0)
            back = back + product(grad_pre, w1, 1, 1)
        out_cells[rows, :] = total
        mid_ref[rows, :] = upstream.astype(f32) + normalize_back(second, scale, back)
        return carry

    lax.fori_loop(0, count // windows, forward, 0)

    mid_low = mid_ref[...].astype(bf16)
    to_tiles(acc1[...], early_in, 0)
    to_tiles(acc2[...].T, early_in, acc1.size // TILE)
    used = 2 * acc1.size // TILE
    to_tiles(product(attn_ref[...], mid_low, 0, 0), early_in, used)
    used += channels * channels // TILE
    if used < early_in.shape[0]:
        early_in[used:] = jnp.zeros((early_in.shape[0] - used, SUB, LANE), bf16)
    for index in early:
        exchange.start(index)
    join_windows(out_cells, grid_ref, mine, order)
    landings = [(rows_land.at[i], cols_land.at[i], corner_land.at[i]) for i in range(2)]
    send_outward(rims[1], rows_pack.at[0], cols_pack.at[0], *landings[0], grid_ref, mine, tile)
    up_ref[...] = product(mid_low, wp_ref[...], 1, 1).astype(bf16)
    scores_ref[...] = jnp.zeros_like(scores_ref)

    def backward(step, carry):
        for slot, moves in enumerate(slots):
            if moves:
                @pl.when(step == slot)
                def _(moves=moves):
                    for index in moves:
                        exchange.advance(index)

        for w in range(PAIR):
            at = pl.ds(pl.multiple_of((step * PAIR + w) * SLOTS, SLOTS), SLOTS)
            for g in range(GROUPS):
                first = slice(g * LANES, (g + 1) * LANES)
                second = slice(channels + g * LANES, channels + (g + 1) * LANES)
                third = slice(2 * channels + g * LANES, 2 * channels + (g + 1) * LANES)
                rows = slice(g * stacked_rows, (g + 1) * stacked_rows)
                query = stack_heads(qkv_ref[at, first], mask_low)
                key = qkv_ref[at, second]
                value = qkv_ref[at, third]
                upstream = stack_heads(up_ref[at, first], mask_low)
                start = ((step * PAIR + w) * GROUPS + g) * stacked_rows
                low = probs_ref[pl.ds(pl.multiple_of(start, stacked_rows), stacked_rows), :]
                probs = low.astype(f32)
                grad_probs = product(upstream, value, 1, 1)
                inner = jnp.sum(probs * grad_probs, -1, keepdims=True)
                grad_scores = probs * (grad_probs - inner)
                scores_ref[rows, :SLOTS] += grad_scores
                scaled = (grad_scores * HEAD_DIM ** (-0.5)).astype(bf16)
                gq_ref[at, first] = gather_heads(product(scaled, key, 1, 0), mask).astype(bf16)
                gq_ref[at, second] = product(scaled, query, 0, 0).astype(bf16)
                gq_ref[at, third] = product(low, upstream, 0, 0).astype(bf16)
        return carry

    lax.fori_loop(0, count // PAIR, backward, 0)

    normal_turned = normal_ref[...].T
    to_tiles(product(normal_turned, gq_ref[...], 1, 0), late_in, 0)
    used = 3 * channels * channels // TILE
    gather_offsets(scores_ref, spread_ref, late_in, used)
    used += CELL
    if used < late_in.shape[0]:
        late_in[used:] = jnp.zeros((late_in.shape[0] - used, SUB, LANE), bf16)
    for index in late:
        exchange.start(index)

    def finish_tokens(step, carry):
        for slot, moves in enumerate(TOKEN_MOVES):
            @pl.when(step == slot)
            def _(moves=moves):
                for index in [index for name in moves for index in (late if name == "l" else early)]:
                    exchange.advance(index)

        rows = pl.ds(pl.multiple_of(step * block, block), block)
        normal, scale = normalize(cell_ref[rows, :channels].astype(f32))
        grad_normed = product(gq_ref[rows, :], wq_ref[...], 1, 1).astype(bf16).astype(f32)
        out_cells[rows, :] = mid_ref[rows, :] + normalize_back(normal, scale, grad_normed)
        return carry

    lax.fori_loop(0, count // windows, finish_tokens, 0)
    join_windows(out_cells, grid_ref, other, order)
    send_outward(rims[2], rows_pack.at[1], cols_pack.at[1], *landings[1], grid_ref, other, tile)
    for index in late + early:
        exchange.advance(index)
    receive_outward(rims[1], *landings[0], grid_ref, mine, tile, out_ref)
    for index in late + early:
        exchange.advance(index)
    receive_outward(rims[2], *landings[1], grid_ref, other, tile, grad_ref)
    exchange.drain(late + early)
    table = jnp.zeros((SUB, 2 * LANE), f32)
    for place in range(CELL):
        table = table + product(late_out[limits[1] + place], picks(offset_ref, place), 1, 1)
    table_out[...] = table
    norm_sq = jnp.sum(square_ref[...]) + jnp.sum(table * table)
    norm_sq = jnp.full((SUB // 2, LANE), norm_sq, f32)
    factor_ref[...] = jnp.minimum(1.0, math.sqrt(PARAMS) / (jnp.sqrt(norm_sq) + 1e-06))
    exchange.close()
    for rim in rims:
        rim.close()


def finish_kernel(
    pieces, block_in, grad_in, early_ref, late_ref, table_ref, factor_ref,
    block_out, token_out, gq_ref, gp_ref, g1_ref, g2_ref, table_out,
    block_full, token_full, tiles, gq_full, gp_full, g1_full, g2_full, in_sem, out_sem,
):
    sources = (early_ref, late_ref)
    results = ((gq_ref, gq_full), (gp_ref, gp_full), (g1_ref, g1_full), (g2_ref, g2_full))
    loads = []
    at = 0
    for i, (group, first, length, _, _, _) in enumerate(pieces):
        load = pltpu.make_async_copy(
            sources[group].at[pl.ds(first, length)], tiles.at[pl.ds(at, length)], in_sem.at[i]
        )
        load.start()
        loads.append((load, at))
        at += length
    passed = ((block_in, block_full, block_out), (grad_in, token_full, token_out))
    for i, (source, full, _) in enumerate(passed):
        load = pltpu.make_async_copy(source, full, in_sem.at[len(pieces) + i])
        load.start()
        loads.append((load, 0))
    factor = factor_ref[:1]
    stores = []
    for i, (group, first, length, which, column, columns) in enumerate(pieces):
        load, at = loads[i]
        load.wait()
        target, full = results[which]
        rows = full.shape[0]
        high = rows // SUB
        for k in range(columns):
            block = tiles[at + k * high : at + (k + 1) * high].reshape(rows, LANE).astype(f32)
            full[:, (column + k) * LANE : (column + k + 1) * LANE] = block * factor
        lanes = pl.ds(column * LANE, columns * LANE)
        store = pltpu.make_async_copy(full.at[:, lanes], target.at[:, lanes], out_sem.at[i])
        store.start()
        stores.append(store)
    for i, (_, full, target) in enumerate(passed):
        loads[len(pieces) + i][0].wait()
        store = pltpu.make_async_copy(full, target, out_sem.at[len(pieces) + i])
        store.start()
        stores.append(store)
    table = table_ref[...] * jnp.concatenate([factor] * 2, 1)
    table_out[...] = table[: table_out.shape[0], : table_out.shape[1]]
    for store in stores:
        store.wait()


def pieces_of(channels, ffn):
    pieces = []
    starts = [0, 0]
    for group, which, rows, lanes, step in (
        (0, 2, channels, ffn, 3), (0, 3, ffn, channels, 1), (0, 1, channels, channels, 3), (1, 0, channels, 3 * channels, 3),
    ):
        for column in range(0, lanes // LANE, step):
            length = rows // SUB * step
            pieces.append((group, starts[group], length, which, column, step))
            starts[group] += length
    return pieces


def local(tokens, cotangent, w_qkv, w_proj, w_fc1, w_fc2, bias_table, rel_index, region):
    tile_rows, tile_cols, channels = tokens.shape
    assert tile_rows == tile_cols and tile_cols + SHIFT < PITCH
    ffn = w_fc1.shape[1]
    count = (tile_rows // SIDE) * (tile_cols // SIDE)
    windows = math.gcd(count, 4)
    total = count * SLOTS

    order, inner = window_order(tile_rows // SIDE, tile_cols // SIDE)
    across = (lax.axis_size("ha"), lax.axis_size("wa"))
    devices = across[0] * across[1]
    early_tiles = padded_tiles((2 * channels * ffn + channels * channels) // TILE, devices)
    late_tiles = padded_tiles(3 * channels * channels // TILE + CELL, devices)
    orders = link_orders(*across)
    streams = split_streams(0, early_tiles, devices, EARLY_PLAN, orders)
    early_count = len(streams)
    streams += split_streams(1, late_tiles, devices, LATE_PLAN, orders)
    slots = slot_moves(early_count, count // PAIR)
    most = max(2 * len(stream[3]) for stream in streams)

    shape = jax.ShapeDtypeStruct
    early = (early_tiles, SUB, LANE)
    late = (late_tiles, SUB, LANE)
    in_vmem = pl.BlockSpec(memory_space=pltpu.VMEM)
    semaphores = pltpu.SemaphoreType.DMA((len(streams), most, 3))
    vmem_limit = 63 * 1024 * 1024
    limits = (early_tiles, 3 * channels * channels // TILE)
    vmem = pltpu.VMEM
    summed = pl.pallas_call(
        functools.partial(block_kernel, windows, streams, slots, limits, order, inner),
        name="block",
        out_shape=[
            shape(tokens.shape, bf16), shape(tokens.shape, bf16), shape(early, bf16), shape(late, bf16),
            shape((SUB, 2 * LANE), f32), shape((SUB // 2, LANE), f32),
        ],
        in_specs=[in_vmem] * 9,
        out_specs=[in_vmem] * 6,
        scratch_shapes=[
            vmem((count, 1, SLOTS), f32),
            vmem((CELL, LANE), jnp.int32),
            vmem((LANE, LANE), f32),
            vmem((LANE, LANE), f32),
            vmem((SUB, 2 * LANE), f32),
            vmem((total, 2 * channels), bf16),
            vmem((2 * channels // LANE, (tile_rows + SHIFT) * PITCH, LANE), f32),
            vmem((total, channels), f32),
            vmem((SUB, LANE), f32),
            vmem((SHIFT, PITCH, 2 * channels), bf16),
            vmem((2, SHIFT, tile_cols, channels), bf16),
            vmem((SHIFT, PITCH, 2 * channels), bf16),
            vmem((SHIFT, SUB, 2 * channels), bf16),
            vmem((2, SHIFT, PITCH, channels), bf16),
            vmem((2, SHIFT, PITCH, channels), bf16),
            vmem((2, SHIFT, PITCH, channels), bf16),
            vmem((2, SHIFT, PITCH, channels), bf16),
            vmem((2, SHIFT, SUB, channels), bf16),
            pltpu.SemaphoreType.DMA((3, 4)),
            pltpu.SemaphoreType.DMA((3, 4)),
            vmem((HEADS * SLOTS, SLOTS), f32),
            vmem((HEADS * CELL, LANE), f32),
            vmem((HEADS * SLOTS, LANE), f32),
            vmem((total, channels), bf16),
            vmem((total, 3 * channels), bf16),
            vmem((total, channels), bf16),
            vmem((count * HEADS * SLOTS, SLOTS), bf16),
            vmem((total, channels), f32),
            vmem((total, channels), bf16),
            vmem((total, 3 * channels), bf16),
            vmem((channels, ffn), f32),
            vmem((channels, ffn), f32),
        ] + [vmem(group, bf16) for group in (early, late)] * 3 + [semaphores] * 2,
        compiler_params=pltpu.CompilerParams(
            collective_id=0, has_side_effects=True, vmem_limit_bytes=vmem_limit
        ),
        cost_estimate=pl.CostEstimate(
            flops=36_000_000_000, bytes_accessed=20_000_000, transcendentals=5_000_000
        ),
    )(tokens, cotangent, region, rel_index, bias_table.T, w_qkv, w_proj, w_fc1, w_fc2)

    pieces = pieces_of(channels, ffn)
    in_place = pl.BlockSpec(memory_space=pl.ANY)
    results = [(channels, 3 * channels), (channels, channels), (channels, ffn), (ffn, channels)]
    block_out, token_grad, gq, gp, g1, g2, table = pl.pallas_call(
        functools.partial(finish_kernel, pieces),
        name="finish",
        out_shape=[shape(tokens.shape, bf16)] * 2
        + [shape(result, f32) for result in results]
        + [shape(bias_table.T.shape, f32)],
        in_specs=[in_place] * 4 + [in_vmem] * 2,
        out_specs=[in_place] * 6 + [in_vmem],
        scratch_shapes=[vmem(tokens.shape, bf16)] * 2
        + [vmem((sum(piece[2] for piece in pieces), SUB, LANE), bf16)]
        + [vmem(result, f32) for result in results]
        + [pltpu.SemaphoreType.DMA((len(pieces) + 2,))] * 2,
        compiler_params=pltpu.CompilerParams(vmem_limit_bytes=vmem_limit),
    )(*summed)
    return (block_out, token_grad, gq, gp, g1, g2, table.T)


def solution(mesh):
    placed = (P("ha", "wa", None), P("ha", "wa", None), P(), P(), P(), P(), P(), P(), P("ha", "wa"))
    return jax.shard_map(
        local,
        mesh=mesh,
        in_specs=placed,
        out_specs=(P("ha", "wa", None), P("ha", "wa", None), P(), P(), P(), P(), P()),
        check_vma=False,
    )
```

```python
import functools
import math

import jax
import jax.numpy as jnp
from jax import lax
from jax.experimental import pallas as pl
from jax.experimental.pallas import tpu as pltpu
from jax.sharding import PartitionSpec as P

HEADS = 12
SIDE = 7
SHIFT = 3
HEAD_DIM = 32
TABLE = 169
PARAMS = 1771500
CELL = 8
SLOTS = CELL * CELL
GROUP = 4
LANES = GROUP * HEAD_DIM
GROUPS = HEADS // GROUP
FFN_CHUNKS = 3
SUB = 16
LANE = 128
TILE = SUB * LANE
EARLY_PLAN = (('a', 4), ('b', 4), ('c', 5), ('a', 4), ('b', 4))
LATE_PLAN = (('d', 1), ('e', 1))
PAIR = 2
TOKEN_MOVES = ('e', 'l', '', 'e')
ROUNDS_BY_SLOT = (0, 1, 1, 1.2, 1.8, 2.4, 3, 3.4)
MESH = pl.DeviceIdType.MESH
PITCH = 32

epsilon = 1e-05
highest = lax.Precision.HIGHEST
f32 = jnp.float32
bf16 = jnp.bfloat16


def normalize(values):
    average = jnp.mean(values, -1, keepdims=True)
    centred = values - average
    inverse = lax.rsqrt(jnp.mean(centred * centred, -1, keepdims=True) + epsilon)
    return (centred * inverse, inverse)


def normalize_back(normal_rows, inverse, upstream):
    up_mean = jnp.mean(upstream, -1, keepdims=True)
    cross_mean = jnp.mean(upstream * normal_rows, -1, keepdims=True)
    return inverse * (upstream - up_mean - normal_rows * cross_mean)


def product(left, right, left_dim, right_dim):
    return lax.dot_general(
        left, right, (((left_dim,), (right_dim,)), ((), ())), preferred_element_type=f32
    )


def head_mask():
    shape = (GROUP * SLOTS, LANES)
    row_head = lax.broadcasted_iota(jnp.int32, shape, 0) // SLOTS
    lane_head = lax.broadcasted_iota(jnp.int32, shape, 1) // HEAD_DIM
    return (row_head == lane_head).astype(f32)


def stack_heads(rows, mask):
    return jnp.concatenate([rows] * GROUP, 0) * mask


def gather_heads(stacked, mask):
    kept = stacked * mask
    total = kept[:SLOTS]
    for head in range(1, GROUP):
        total = total + kept[head * SLOTS : (head + 1) * SLOTS]
    return total


def to_tiles(values, tiles_ref, at):
    rows, lanes = values.shape
    high = rows // SUB
    low = values.astype(bf16)
    for column in range(lanes // LANE):
        block = low[:, column * LANE : (column + 1) * LANE].reshape(high, SUB, LANE)
        tiles_ref[at + column * high : at + (column + 1) * high] = block


def digits_of(axis, size, stride, most):
    digits = []
    while stride < size:
        radix = min(most, size // stride)
        digits.append((axis, stride, radix))
        stride *= radix
    return digits


def link_orders(across_ha, across_wa):
    core = digits_of("wa", 2, 1, 2)
    near = digits_of("ha", across_ha, 1, 2)
    near_wide = digits_of("ha", across_ha, 1, 4)
    far = digits_of("wa", across_wa, 2, 4)
    far_slim = digits_of("wa", across_wa, 2, 2)
    orders = {
        "a": core + near + far,
        "b": core + near[::-1] + far,
        "c": core + far + near,
        "d": core + near_wide + far,
        "e": core + far + near_wide,
        "s": core + near + far_slim,
        "t": core + near[::-1] + far_slim,
        "u": core + far_slim + near,
    }
    return orders


def split_streams(group, tiles, devices, plan, orders):
    units = tiles // devices
    total = sum(weight for _, weight in plan)
    streams = []
    base = 0
    passed = 0
    for name, weight in plan:
        passed += weight
        size = (units * passed + total // 2) // total * devices - base
        if size:
            streams.append((group, base, size, orders[name]))
        base += size
    return streams


def slot_moves(streams, slots):
    moves = []
    done = 0
    for slot in range(slots):
        until = int(ROUNDS_BY_SLOT[min(slot, len(ROUNDS_BY_SLOT) - 1)] * streams)
        moves.append([index % streams for index in range(done, until)])
        done = max(done, until)
    return moves


def padded_tiles(tiles, devices):
    return -(-tiles // devices) * devices


def chunk_of(count):
    return max(size for size in range(1, 17) if count % size == 0)


class Exchange:
    def __init__(self, streams, sources, sums, landing, totals, send_sem, recv_sem, limits, square_ref):
        self.streams = streams
        self.sources, self.sums, self.landing, self.totals = sources, sums, landing, totals
        self.send_sem, self.recv_sem = send_sem, recv_sem
        self.limits, self.square_ref = limits, square_ref
        self.done = [0] * len(streams)
        self.places = []
        self.partners = {}
        for group, base, size, order in streams:
            places = []
            low = base
            arrive = base
            for axis, stride, radix in order:
                size = size // radix
                me = lax.axis_index(axis)
                digit = (me // stride) % radix
                sends = []
                for k in range(1, radix):
                    ahead = (digit + k) % radix
                    behind = (digit + radix - k) % radix
                    partner = {axis: me + (ahead - digit) * stride}
                    self.partners[axis, stride, radix, k] = partner
                    sends.append((partner, low + ahead * size, low + behind * size, arrive))
                    arrive += size
                low = low + digit * size
                places.append((low, size, sends))
            self.places.append(places)

    def rounds(self, index):
        return len(self.places[index])

    def copies(self, index, slot):
        group = self.streams[index][0]
        rounds = self.rounds(index)
        keep, size, sends = self.places[index][slot if slot < rounds else 2 * rounds - 1 - slot]
        result = []
        for k, (partner, give, _, arrive) in enumerate(sends):
            if slot < rounds:
                source = (self.sums if slot else self.sources)[group].at[pl.ds(give, size)]
                target = self.landing[group].at[pl.ds(arrive, size)]
            else:
                source = self.totals[group].at[pl.ds(keep, size)]
                target = source
            result.append(
                pltpu.make_async_remote_copy(
                    src_ref=source,
                    dst_ref=target,
                    send_sem=self.send_sem.at[index, slot, k],
                    recv_sem=self.recv_sem.at[index, slot, k],
                    device_id=partner,
                    device_id_type=MESH,
                )
            )
        return result

    def add(self, index, step):
        group = self.streams[index][0]
        keep, size, sends = self.places[index][step]
        source = (self.sums if step else self.sources)[group]
        target = (self.sums if step < self.rounds(index) - 1 else self.totals)[group]
        landing = self.landing[group]
        chunk = chunk_of(size)

        def body(i, carry):
            at = pl.ds(keep + i * chunk, chunk)
            total = source[at].astype(f32)
            for _, _, _, arrive in sends:
                total = total + landing[pl.ds(arrive + i * chunk, chunk)].astype(f32)
            target[at] = total.astype(bf16)
            return carry

        lax.fori_loop(0, size // chunk, body, 0)

    def start(self, index, slot=0):
        for copy in self.copies(index, slot):
            copy.start()

    def advance(self, index):
        slot = self.done[index]
        rounds = self.rounds(index)
        if slot == 2 * rounds:
            return
        for copy in self.copies(index, slot):
            copy.wait_recv()
        if slot < rounds:
            self.add(index, slot)
        if slot + 1 < 2 * rounds:
            self.start(index, slot + 1)
        keep, size, sends = self.places[index][slot if slot < rounds else 2 * rounds - 1 - slot]
        if slot == rounds - 1:
            self.square(index, keep, size)
        elif slot >= rounds:
            for _, _, behind, _ in sends:
                self.square(index, behind, size)
        self.done[index] = slot + 1

    def square(self, index, first, length):
        group = self.streams[index][0]
        totals = self.totals[group]
        chunk = chunk_of(length)

        def body(i, total):
            at = first + i * chunk
            block = totals[pl.ds(at, chunk)].astype(f32)
            inside = lax.broadcasted_iota(jnp.int32, block.shape, 0) + at < self.limits[group]
            return total + jnp.sum(jnp.where(inside, block * block, 0.0), 0)

        total = lax.fori_loop(0, length // chunk, body, jnp.zeros((SUB, LANE), f32))
        self.square_ref[...] += total

    def drain(self, order):
        while any(self.done[index] < 2 * self.rounds(index) for index in order):
            for index in order:
                self.advance(index)

    def close(self):
        for index in range(len(self.streams)):
            for slot in range(2 * self.rounds(index)):
                for copy in self.copies(index, slot):
                    copy.wait_send()


class Rims:
    def __init__(self, by, send_sem, recv_sem, phase):
        spots = {}
        for axis in ("ha", "wa"):
            count = lax.axis_size(axis)
            spots[axis] = (lax.axis_index(axis) + by + count) % count
        self.targets = ({"ha": spots["ha"]}, {"wa": spots["wa"]}, spots)
        self.send_sem, self.recv_sem, self.phase = send_sem, recv_sem, phase
        self.copies = []

    def send(self, which, source, target):
        at = (self.phase, len(self.copies))
        copy = pltpu.make_async_remote_copy(
            src_ref=source,
            dst_ref=target,
            send_sem=self.send_sem.at[at],
            recv_sem=self.recv_sem.at[at],
            device_id=self.targets[which],
            device_id_type=MESH,
        )
        copy.start()
        self.copies.append(copy)

    def receive(self):
        for copy in self.copies:
            copy.wait_recv()

    def close(self):
        for copy in self.copies:
            copy.wait_send()


def greet(partners):
    barrier = pltpu.get_barrier_semaphore()
    for partner in partners:
        pl.semaphore_signal(barrier, inc=1, device_id=partner, device_id_type=MESH)


def column_of(grid_ref, first, height, layers):
    return jnp.concatenate([grid_ref[layer, pl.ds(first, height, stride=PITCH), :] for layer in layers], 1)


def put_column(grid_ref, first, layers, values):
    for i, layer in enumerate(layers):
        part = values[:, i * LANE : (i + 1) * LANE]
        grid_ref[layer, pl.ds(first, values.shape[0], stride=PITCH), :] = part


def rows_at(grid_ref, first, height, layers):
    return jnp.concatenate([grid_ref[layer, first : first + height, :] for layer in layers], 1)


def put_rows(grid_ref, first, layers, values):
    for i, layer in enumerate(layers):
        grid_ref[layer, first : first + values.shape[0], :] = values[:, i * LANE : (i + 1) * LANE]


def padded_column(column):
    filler = jnp.zeros((PITCH - column.shape[0], column.shape[1]), f32)
    return jnp.concatenate([column, filler], 0).astype(bf16)


def send_outward(rims, rows_ref, cols_ref, rows_land, cols_land, corner_land, grid_ref, layers, tile):
    for k in range(SHIFT):
        rows_ref[k] = rows_at(grid_ref, (tile + k) * PITCH, PITCH, layers).astype(bf16)
        cols_ref[k] = padded_column(column_of(grid_ref, tile + k, tile + SHIFT, layers))
    rims.send(0, rows_ref, rows_land)
    rims.send(1, cols_ref, cols_land)
    rims.send(2, rows_ref.at[:, pl.ds(PITCH - SUB, SUB)], corner_land)


def receive_outward(rims, rows_land, cols_land, corner_land, grid_ref, layers, tile, target_ref):
    rims.receive()
    corner = tile - (PITCH - SUB)
    for k in range(SHIFT):
        put_rows(grid_ref, k * PITCH, layers, rows_land[k].astype(f32))
    for k in range(SHIFT):
        put_column(grid_ref, k, layers, cols_land[k].astype(f32)[: tile + SHIFT])
    for k in range(SHIFT):
        put_rows(grid_ref, k * PITCH, layers, corner_land[k].astype(f32)[corner : corner + SHIFT])
    for row in range(tile):
        target_ref[row] = rows_at(grid_ref, row * PITCH, tile, layers).astype(bf16)


def window_order(rows, cols):
    spots = [(row, col) for row in range(rows) for col in range(cols)]
    inner = [spot for spot in spots if spot[0] < rows - 1 and spot[1] < cols - 1]
    return inner + [spot for spot in spots if spot not in inner], len(inner)


def pack_rows(values):
    count = values.shape[0] // SLOTS
    return jnp.concatenate([values[w * SLOTS : w * SLOTS + SIDE * CELL] for w in range(count)], 0)


def unpack_rows(values):
    height = SIDE * CELL
    filler = jnp.zeros((SLOTS - height, values.shape[1]), values.dtype)
    parts = []
    for w in range(values.shape[0] // height):
        parts += [values[w * height : (w + 1) * height], filler]
    return jnp.concatenate(parts, 0)


def place_of(spot, row):
    return (spot[0] * SIDE + row + SHIFT) * PITCH + spot[1] * SIDE + SHIFT


def cut_windows(grid_ref, cell_ref, order, first, last):
    inside = lax.broadcasted_iota(jnp.int32, (CELL, LANE), 0) < SIDE
    for window in range(first, last):
        for layer in range(grid_ref.shape[0]):
            rows = []
            for row in range(SIDE):
                at = place_of(order[window], row)
                rows.append(jnp.where(inside, grid_ref[layer, at : at + CELL, :], 0.0))
            rows.append(jnp.zeros_like(rows[0]))
            lanes = slice(layer * LANE, (layer + 1) * LANE)
            cell_ref[window * SLOTS : (window + 1) * SLOTS, lanes] = jnp.concatenate(rows, 0).astype(bf16)


def join_windows(values, grid_ref, layers, order):
    for window, spot in enumerate(order):
        for row in range(SIDE):
            place = window * SLOTS + row * CELL
            put_rows(grid_ref, place_of(spot, row), layers, values[place : place + SIDE])


def fill_labels(region_ref, wide_ref, label_ref, order):
    rows, cols = region_ref.shape
    wide_ref[:rows, :cols] = region_ref[...].astype(f32)
    area = wide_ref[: -(-rows // CELL) * CELL, :]
    lane = lax.broadcasted_iota(jnp.int32, (1, LANE), 1)
    labels = [jnp.full((1, LANE), -1.0, f32) for _ in order]
    for col in range(cols // SIDE):
        for row in range(SIDE):
            turned = pltpu.roll(area, (row * CELL - col * SIDE) % LANE, 1)
            inside = (lane >= row * CELL) & (lane < row * CELL + SIDE)
            for window, spot in enumerate(order):
                if spot[1] == col:
                    at = spot[0] * SIDE + row
                    labels[window] = jnp.where(inside, turned[at : at + 1, :], labels[window])
    for window in range(len(order)):
        label_ref[window] = labels[window][:, :SLOTS]


def fill_offsets(rel_ref, wide_ref, offset_ref):
    size = rel_ref.shape[0]
    wide_ref[:size, :size] = rel_ref[...].astype(f32)
    lane = lax.broadcasted_iota(jnp.int32, (CELL, LANE), 1)
    row = lax.broadcasted_iota(jnp.int32, (CELL, LANE), 0)
    result = jnp.full((CELL, LANE), -1.0, f32)
    for offset in range(1 - SIDE, SIDE):
        if offset < 0:
            turned = pltpu.roll(wide_ref[-offset * SIDE : CELL - offset * SIDE, :], (SIDE + offset) * CELL, 1)
        else:
            turned = pltpu.roll(wide_ref[:CELL, :], (SIDE + offset) * CELL - offset * SIDE, 1)
        first = (SIDE + offset) * CELL
        result = jnp.where((lane >= first) & (lane < first + SIDE), turned, result)
    offset_ref[...] = jnp.where(row < SIDE, result, -1.0).astype(jnp.int32)


def picks(offset_ref, place):
    labels = lax.broadcasted_iota(jnp.int32, (2 * LANE, LANE), 0)
    return (labels == offset_ref[place : place + 1, :]).astype(f32).astype(bf16)


def fill_bias(offset_ref, table_ref, wide_ref, spread_ref, bias_ref):
    wide_ref[: table_ref.shape[0], : table_ref.shape[1]] = table_ref[...]
    rest = wide_ref[...]
    parts = []
    for _ in range(3):
        part = rest.astype(bf16)
        parts.append(part)
        rest = rest - part.astype(f32)
    parts = jnp.concatenate(parts, 0)
    for place in range(CELL):
        spread = product(parts, picks(offset_ref, place), 1, 0)
        spread = spread[:SUB] + (spread[SUB : 2 * SUB] + spread[2 * SUB :])
        spread_ref[pl.ds(place, HEADS, stride=CELL), :] = spread[:HEADS]
    for head in range(HEADS):
        rows = spread_ref[head * CELL : (head + 1) * CELL, :]
        for row in range(CELL):
            at = head * SLOTS + row * CELL
            if row < SIDE:
                turned = pltpu.roll(rows, LANE - (SIDE - row) * CELL, 1)
                bias_ref[at : at + CELL, :] = turned[:, :SLOTS]
            else:
                bias_ref[at : at + CELL, :] = jnp.zeros((CELL, SLOTS), f32)


def gather_offsets(scores_ref, spread_ref, tiles_ref, first):
    for head in range(HEADS):
        total = jnp.zeros((CELL, LANE), f32)
        for row in range(SIDE):
            at = head * SLOTS + row * CELL
            total = total + pltpu.roll(scores_ref[at : at + CELL, :], (SIDE - row) * CELL, 1)
        spread_ref[head * CELL : (head + 1) * CELL, :] = total
    for place in range(CELL):
        rows = spread_ref[pl.ds(place, HEADS, stride=CELL), :]
        rows = jnp.concatenate([rows, jnp.zeros((SUB - HEADS, LANE), f32)], 0)
        tiles_ref[first + place] = rows.astype(bf16)


def block_kernel(
    windows, streams, slots, limits, order, inner,
    tok_ref, ct_ref, region_in, rel_ref, table_in, wq_in, wp_in, w1_in, w2_in,
    out_ref, grad_ref, early_out, late_out, table_out, factor_ref,
    wq_ref, wp_ref, w1_ref, w2_ref, weight_sem, region_ref, offset_ref, wide_region, wide_rel, wide_table, cell_ref, grid_ref, out_cells, square_ref, in_cols, in_land, in_cols_land, in_corner_land,
    rows_pack, cols_pack, rows_land, cols_land, corner_land, rim_send, rim_recv,
    bias_ref, spread_ref, scores_ref, normal_ref, qkv_ref, attn_ref, probs_ref, mid_ref, up_ref, gq_ref,
    acc1, acc2, early_in, late_in, early_sum, late_sum, early_land, late_land, send_sem, recv_sem,
):
    exchange = Exchange(
        streams, (early_in, late_in), (early_sum, late_sum), (early_land, late_land), (early_out, late_out),
        send_sem, recv_sem, limits, square_ref,
    )
    rims = [Rims(by, rim_send, rim_recv, phase) for phase, by in enumerate((-1, 1, 1))]
    partners = list(exchange.partners.values()) + list(rims[0].targets) + list(rims[1].targets)
    greet(partners)
    early = [index for index, stream in enumerate(streams) if stream[0] == 0]
    late = [index for index, stream in enumerate(streams) if stream[0] == 1]
    weights = [
        pltpu.make_async_copy(source, target, weight_sem.at[i])
        for i, (source, target) in enumerate(((wq_in, wq_ref), (wp_in, wp_ref), (w1_in, w1_ref), (w2_in, w2_ref)))
    ]
    for weight in weights:
        weight.start()
    tile, _, channels = tok_ref.shape
    count = cell_ref.shape[0] // SLOTS
    block = windows * SLOTS
    hidden_units = w1_ref.shape[1]
    width = hidden_units // FFN_CHUNKS
    stacked_rows = GROUP * SLOTS
    mask = head_mask()
    mask_low = mask.astype(bf16)
    mine = range(channels // LANE)
    other = range(channels // LANE, 2 * channels // LANE)
    both = range(2 * channels // LANE)
    for row in range(tile):
        put_rows(grid_ref, row * PITCH, mine, tok_ref[row].astype(f32))
        put_rows(grid_ref, row * PITCH, other, ct_ref[row].astype(f32))
    for k in range(SHIFT):
        in_cols[k] = padded_column(column_of(grid_ref, k, tile, both))
    for wide_ref in (wide_region, wide_rel, wide_table):
        wide_ref[...] = jnp.zeros_like(wide_ref)
    fill_labels(region_in, wide_region, region_ref, order)
    fill_offsets(rel_ref, wide_rel, offset_ref)
    fill_bias(offset_ref, table_in, wide_table, spread_ref, bias_ref)
    square_ref[...] = jnp.zeros_like(square_ref)
    pl.semaphore_wait(pltpu.get_barrier_semaphore(), len(partners))
    rims[0].send(0, tok_ref.at[pl.ds(0, SHIFT)], in_land.at[0])
    rims[0].send(0, ct_ref.at[pl.ds(0, SHIFT)], in_land.at[1])
    rims[0].send(1, in_cols, in_cols_land)
    rims[0].send(2, in_cols.at[:, pl.ds(0, SUB)], in_corner_land)
    ready = inner // windows
    cut_windows(grid_ref, cell_ref, order, 0, ready * windows)

    def take_rims():
        rims[0].receive()
        for k in range(SHIFT):
            put_rows(grid_ref, (tile + k) * PITCH, mine, in_land[0, k].astype(f32))
            put_rows(grid_ref, (tile + k) * PITCH, other, in_land[1, k].astype(f32))
            put_column(grid_ref, tile + k, both, in_cols_land[k].astype(f32)[:tile])
            put_column(grid_ref, tile * PITCH + tile + k, both, in_corner_land[k].astype(f32)[:SHIFT])
        cut_windows(grid_ref, cell_ref, order, ready * windows, count)

    for weight in weights:
        weight.wait()
    acc1[...] = jnp.zeros_like(acc1)
    acc2[...] = jnp.zeros_like(acc2)

    def forward(step, carry):
        pl.when(step == ready)(take_rims)
        rows = pl.ds(pl.multiple_of(step * block, block), block)
        token = cell_ref[rows, :channels].astype(f32)
        upstream = pack_rows(cell_ref[rows, channels:].astype(f32)).astype(bf16)
        normal, _ = normalize(token)
        normal_low = normal.astype(bf16)
        normal_ref[rows, :] = normal_low
        qkv_ref[rows, :] = product(normal_low, wq_ref[...], 1, 0).astype(bf16)
        for w in range(windows):
            at = pl.ds(pl.multiple_of(step * block + w * SLOTS, SLOTS), SLOTS)
            labels = jnp.broadcast_to(region_ref[step * windows + w], (SLOTS, SLOTS))
            hidden = jnp.where(labels == labels.T, 0.0, -1e30)
            hidden = jnp.concatenate([hidden] * GROUP, 0)
            for g in range(GROUPS):
                lanes = g * LANES
                query = stack_heads(qkv_ref[at, lanes : lanes + LANES], mask_low)
                key = qkv_ref[at, channels + lanes : channels + lanes + LANES]
                value = qkv_ref[at, 2 * channels + lanes : 2 * channels + lanes + LANES]
                bias = bias_ref[g * stacked_rows : (g + 1) * stacked_rows, :]
                scores = product(query, key, 1, 1) * HEAD_DIM ** (-0.5) + bias + hidden
                exponent = jnp.exp(scores - jnp.max(scores, -1, keepdims=True))
                probs = (exponent * (1.0 / jnp.sum(exponent, -1, keepdims=True))).astype(bf16)
                start = ((step * windows + w) * GROUPS + g) * stacked_rows
                probs_ref[pl.ds(pl.multiple_of(start, stacked_rows), stacked_rows), :] = probs
                mixed = product(probs, value, 1, 0)
                attn_ref[at, lanes : lanes + LANES] = gather_heads(mixed, mask).astype(bf16)
        projected = product(attn_ref[rows, :], wp_ref[...], 1, 0).astype(bf16)
        middle = pack_rows(token + projected.astype(f32))
        second, scale = normalize(middle)
        low = second.astype(bf16)
        low_turned = low.T
        up_turned = upstream.T
        total = middle
        back = jnp.zeros_like(middle)
        for c in range(FFN_CHUNKS):
            at = slice(c * width, (c + 1) * width)
            w1 = w1_ref[:, at]
            w2 = w2_ref[at, :]
            pre = product(low, w1, 1, 0)
            cdf = 0.5 * (1.0 + lax.erf(pre * 2.0 ** (-0.5)))
            density = jnp.exp(-0.5 * pre * pre) * (2.0 * math.pi) ** (-0.5)
            active = (pre * cdf).astype(bf16)
            total = total + product(active, w2, 1, 0)
            acc2[:, at] += product(up_turned, active, 1, 0)
            grad_pre = (product(upstream, w2, 1, 1) * (cdf + pre * density)).astype(bf16)
            acc1[:, at] += product(low_turned, grad_pre, 1, 0)
            back = back + product(grad_pre, w1, 1, 1)
        out_cells[rows, :] = unpack_rows(total)
        mid_ref[rows, :] = unpack_rows(upstream.astype(f32) + normalize_back(second, scale, back))
        return carry

    lax.fori_loop(0, count // windows, forward, 0)

    mid_low = mid_ref[...].astype(bf16)
    to_tiles(acc1[...], early_in, 0)
    to_tiles(acc2[...].T, early_in, acc1.size // TILE)
    used = 2 * acc1.size // TILE
    to_tiles(product(attn_ref[...], mid_low, 0, 0), early_in, used)
    used += channels * channels // TILE
    if used < early_in.shape[0]:
        early_in[used:] = jnp.zeros((early_in.shape[0] - used, SUB, LANE), bf16)
    for index in early:
        exchange.start(index)
    join_windows(out_cells, grid_ref, mine, order)
    landings = [(rows_land.at[i], cols_land.at[i], corner_land.at[i]) for i in range(2)]
    send_outward(rims[1], rows_pack.at[0], cols_pack.at[0], *landings[0], grid_ref, mine, tile)
    up_ref[...] = product(mid_low, wp_ref[...], 1, 1).astype(bf16)
    scores_ref[...] = jnp.zeros_like(scores_ref)

    def backward(step, carry):
        for slot, moves in enumerate(slots):
            if moves:
                @pl.when(step == slot)
                def _(moves=moves):
                    for index in moves:
                        exchange.advance(index)

        for w in range(PAIR):
            at = pl.ds(pl.multiple_of((step * PAIR + w) * SLOTS, SLOTS), SLOTS)
            for g in range(GROUPS):
                first = slice(g * LANES, (g + 1) * LANES)
                second = slice(channels + g * LANES, channels + (g + 1) * LANES)
                third = slice(2 * channels + g * LANES, 2 * channels + (g + 1) * LANES)
                rows = slice(g * stacked_rows, (g + 1) * stacked_rows)
                query = stack_heads(qkv_ref[at, first], mask_low)
                key = qkv_ref[at, second]
                value = qkv_ref[at, third]
                upstream = stack_heads(up_ref[at, first], mask_low)
                start = ((step * PAIR + w) * GROUPS + g) * stacked_rows
                low = probs_ref[pl.ds(pl.multiple_of(start, stacked_rows), stacked_rows), :]
                probs = low.astype(f32)
                grad_probs = product(upstream, value, 1, 1)
                inner = jnp.sum(probs * grad_probs, -1, keepdims=True)
                grad_scores = probs * (grad_probs - inner)
                scores_ref[rows, :SLOTS] += grad_scores
                scaled = (grad_scores * HEAD_DIM ** (-0.5)).astype(bf16)
                gq_ref[at, first] = gather_heads(product(scaled, key, 1, 0), mask).astype(bf16)
                gq_ref[at, second] = product(scaled, query, 0, 0).astype(bf16)
                gq_ref[at, third] = product(low, upstream, 0, 0).astype(bf16)
        return carry

    lax.fori_loop(0, count // PAIR, backward, 0)

    normal_turned = normal_ref[...].T
    to_tiles(product(normal_turned, gq_ref[:, : 2 * channels], 1, 0), late_in, 0)
    used = 2 * channels * channels // TILE
    first_late = [index for index in late if streams[index][1] + streams[index][2] <= used]
    for index in first_late:
        exchange.start(index)
    to_tiles(product(normal_turned, gq_ref[:, 2 * channels :], 1, 0), late_in, used)
    used = 3 * channels * channels // TILE
    gather_offsets(scores_ref, spread_ref, late_in, used)
    used += CELL
    if used < late_in.shape[0]:
        late_in[used:] = jnp.zeros((late_in.shape[0] - used, SUB, LANE), bf16)
    for index in late:
        if index not in first_late:
            exchange.start(index)

    def finish_tokens(step, carry):
        for slot, moves in enumerate(TOKEN_MOVES):
            @pl.when(step == slot)
            def _(moves=moves):
                for index in [index for name in moves for index in (late if name == "l" else early)]:
                    exchange.advance(index)

        rows = pl.ds(pl.multiple_of(step * block, block), block)
        normal, scale = normalize(cell_ref[rows, :channels].astype(f32))
        grad_normed = product(gq_ref[rows, :], wq_ref[...], 1, 1).astype(bf16).astype(f32)
        out_cells[rows, :] = mid_ref[rows, :] + normalize_back(normal, scale, grad_normed)
        return carry

    lax.fori_loop(0, count // windows, finish_tokens, 0)
    join_windows(out_cells, grid_ref, other, order)
    send_outward(rims[2], rows_pack.at[1], cols_pack.at[1], *landings[1], grid_ref, other, tile)
    for index in late + early:
        exchange.advance(index)
    receive_outward(rims[1], *landings[0], grid_ref, mine, tile, out_ref)
    for index in late + early:
        exchange.advance(index)
    receive_outward(rims[2], *landings[1], grid_ref, other, tile, grad_ref)
    exchange.drain(late + early)
    table = jnp.zeros((SUB, 2 * LANE), f32)
    for place in range(CELL):
        table = table + product(late_out[limits[1] + place], picks(offset_ref, place), 1, 1)
    table_out[...] = table
    norm_sq = jnp.sum(square_ref[...]) + jnp.sum(table * table)
    norm_sq = jnp.full((SUB // 2, LANE), norm_sq, f32)
    factor_ref[...] = jnp.minimum(1.0, math.sqrt(PARAMS) / (jnp.sqrt(norm_sq) + 1e-06))
    exchange.close()
    for rim in rims:
        rim.close()


def finish_kernel(
    pieces, block_in, grad_in, early_ref, late_ref, table_ref, factor_ref,
    block_out, token_out, gq_ref, gp_ref, g1_ref, g2_ref, table_out,
    block_full, token_full, tiles, gq_full, gp_full, g1_full, g2_full, in_sem, out_sem,
):
    sources = (early_ref, late_ref)
    results = ((gq_ref, gq_full), (gp_ref, gp_full), (g1_ref, g1_full), (g2_ref, g2_full))
    loads = []
    at = 0
    for i, (group, first, length, _, _, _) in enumerate(pieces):
        load = pltpu.make_async_copy(
            sources[group].at[pl.ds(first, length)], tiles.at[pl.ds(at, length)], in_sem.at[i]
        )
        load.start()
        loads.append((load, at))
        at += length
    passed = ((block_in, block_full, block_out), (grad_in, token_full, token_out))
    for i, (source, full, _) in enumerate(passed):
        load = pltpu.make_async_copy(source, full, in_sem.at[len(pieces) + i])
        load.start()
        loads.append((load, 0))
    factor = factor_ref[:1]
    stores = []
    for i, (group, first, length, which, column, columns) in enumerate(pieces):
        load, at = loads[i]
        load.wait()
        target, full = results[which]
        rows = full.shape[0]
        high = rows // SUB
        for k in range(columns):
            block = tiles[at + k * high : at + (k + 1) * high].reshape(rows, LANE).astype(f32)
            full[:, (column + k) * LANE : (column + k + 1) * LANE] = block * factor
        lanes = pl.ds(column * LANE, columns * LANE)
        store = pltpu.make_async_copy(full.at[:, lanes], target.at[:, lanes], out_sem.at[i])
        store.start()
        stores.append(store)
    for i, (_, full, target) in enumerate(passed):
        loads[len(pieces) + i][0].wait()
        store = pltpu.make_async_copy(full, target, out_sem.at[len(pieces) + i])
        store.start()
        stores.append(store)
    table = table_ref[...] * jnp.concatenate([factor] * 2, 1)
    table_out[...] = table[: table_out.shape[0], : table_out.shape[1]]
    for store in stores:
        store.wait()


def pieces_of(channels, ffn):
    pieces = []
    starts = [0, 0]
    for group, which, rows, lanes, step in (
        (0, 2, channels, ffn, 3), (0, 3, ffn, channels, 1), (0, 1, channels, channels, 3), (1, 0, channels, 3 * channels, 3),
    ):
        for column in range(0, lanes // LANE, step):
            length = rows // SUB * step
            pieces.append((group, starts[group], length, which, column, step))
            starts[group] += length
    return pieces


def local(tokens, cotangent, w_qkv, w_proj, w_fc1, w_fc2, bias_table, rel_index, region):
    tile_rows, tile_cols, channels = tokens.shape
    assert tile_rows == tile_cols and tile_cols + SHIFT < PITCH
    ffn = w_fc1.shape[1]
    count = (tile_rows // SIDE) * (tile_cols // SIDE)
    windows = math.gcd(count, 4)
    total = count * SLOTS

    order, inner = window_order(tile_rows // SIDE, tile_cols // SIDE)
    across = (lax.axis_size("ha"), lax.axis_size("wa"))
    devices = across[0] * across[1]
    early_tiles = padded_tiles((2 * channels * ffn + channels * channels) // TILE, devices)
    late_tiles = padded_tiles(3 * channels * channels // TILE + CELL, devices)
    orders = link_orders(*across)
    streams = split_streams(0, early_tiles, devices, EARLY_PLAN, orders)
    early_count = len(streams)
    streams += split_streams(1, late_tiles, devices, LATE_PLAN, orders)
    slots = slot_moves(early_count, count // PAIR)
    most = max(2 * len(stream[3]) for stream in streams)

    shape = jax.ShapeDtypeStruct
    early = (early_tiles, SUB, LANE)
    late = (late_tiles, SUB, LANE)
    in_vmem = pl.BlockSpec(memory_space=pltpu.VMEM)
    semaphores = pltpu.SemaphoreType.DMA((len(streams), most, 3))
    vmem_limit = 63 * 1024 * 1024
    limits = (early_tiles, 3 * channels * channels // TILE)
    vmem = pltpu.VMEM
    summed = pl.pallas_call(
        functools.partial(block_kernel, windows, streams, slots, limits, order, inner),
        name="block",
        out_shape=[
            shape(tokens.shape, bf16), shape(tokens.shape, bf16), shape(early, bf16), shape(late, bf16),
            shape((SUB, 2 * LANE), f32), shape((SUB // 2, LANE), f32),
        ],
        in_specs=[in_vmem] * 5 + [pl.BlockSpec(memory_space=pl.ANY)] * 4,
        out_specs=[in_vmem] * 6,
        scratch_shapes=[
            vmem(w_qkv.shape, bf16),
            vmem(w_proj.shape, bf16),
            vmem(w_fc1.shape, bf16),
            vmem(w_fc2.shape, bf16),
            pltpu.SemaphoreType.DMA((4,)),
            vmem((count, 1, SLOTS), f32),
            vmem((CELL, LANE), jnp.int32),
            vmem((LANE, LANE), f32),
            vmem((LANE, LANE), f32),
            vmem((SUB, 2 * LANE), f32),
            vmem((total, 2 * channels), bf16),
            vmem((2 * channels // LANE, (tile_rows + SHIFT) * PITCH, LANE), f32),
            vmem((total, channels), f32),
            vmem((SUB, LANE), f32),
            vmem((SHIFT, PITCH, 2 * channels), bf16),
            vmem((2, SHIFT, tile_cols, channels), bf16),
            vmem((SHIFT, PITCH, 2 * channels), bf16),
            vmem((SHIFT, SUB, 2 * channels), bf16),
            vmem((2, SHIFT, PITCH, channels), bf16),
            vmem((2, SHIFT, PITCH, channels), bf16),
            vmem((2, SHIFT, PITCH, channels), bf16),
            vmem((2, SHIFT, PITCH, channels), bf16),
            vmem((2, SHIFT, SUB, channels), bf16),
            pltpu.SemaphoreType.DMA((3, 4)),
            pltpu.SemaphoreType.DMA((3, 4)),
            vmem((HEADS * SLOTS, SLOTS), f32),
            vmem((HEADS * CELL, LANE), f32),
            vmem((HEADS * SLOTS, LANE), f32),
            vmem((total, channels), bf16),
            vmem((total, 3 * channels), bf16),
            vmem((total, channels), bf16),
            vmem((count * HEADS * SLOTS, SLOTS), bf16),
            vmem((total, channels), f32),
            vmem((total, channels), bf16),
            vmem((total, 3 * channels), bf16),
            vmem((channels, ffn), f32),
            vmem((channels, ffn), f32),
        ] + [vmem(group, bf16) for group in (early, late)] * 3 + [semaphores] * 2,
        compiler_params=pltpu.CompilerParams(
            collective_id=0, has_side_effects=True, vmem_limit_bytes=vmem_limit
        ),
        cost_estimate=pl.CostEstimate(
            flops=36_000_000_000, bytes_accessed=20_000_000, transcendentals=5_000_000
        ),
    )(tokens, cotangent, region, rel_index, bias_table.T, w_qkv, w_proj, w_fc1, w_fc2)

    pieces = pieces_of(channels, ffn)
    in_place = pl.BlockSpec(memory_space=pl.ANY)
    results = [(channels, 3 * channels), (channels, channels), (channels, ffn), (ffn, channels)]
    block_out, token_grad, gq, gp, g1, g2, table = pl.pallas_call(
        functools.partial(finish_kernel, pieces),
        name="finish",
        out_shape=[shape(tokens.shape, bf16)] * 2
        + [shape(result, f32) for result in results]
        + [shape(bias_table.T.shape, f32)],
        in_specs=[in_place] * 4 + [in_vmem] * 2,
        out_specs=[in_place] * 6 + [in_vmem],
        scratch_shapes=[vmem(tokens.shape, bf16)] * 2
        + [vmem((sum(piece[2] for piece in pieces), SUB, LANE), bf16)]
        + [vmem(result, f32) for result in results]
        + [pltpu.SemaphoreType.DMA((len(pieces) + 2,))] * 2,
        compiler_params=pltpu.CompilerParams(vmem_limit_bytes=vmem_limit),
    )(*summed)
    return (block_out, token_grad, gq, gp, g1, g2, table.T)


def solution(mesh):
    placed = (P("ha", "wa", None), P("ha", "wa", None), P(), P(), P(), P(), P(), P(), P("ha", "wa"))
    return jax.shard_map(
        local,
        mesh=mesh,
        in_specs=placed,
        out_specs=(P("ha", "wa", None), P("ha", "wa", None), P(), P(), P(), P(), P()),
        check_vma=False,
    )
```
